32 devices in a mesh: groups: 2 (over x), seq: 8 (over z, y), expert: 2 (over core).
Axes of the slice: x: 2, y: 2, z: 4, core: 2. Of those that a mesh axis runs over, the one named last changes fastest.
Arguments:
- residual: bfloat16 [8, 6144], P('groups', 'seq'), parts along dimension 0, may hold values from -27 to 27
- queries: bfloat16 [8, 6144], P('groups', 'expert'), parts along dimension 0, may hold values from -6 to 6
- new_entries: bfloat16 [2, 8, 1024], P(None, 'groups', 'expert'), parts along dimension 1, may hold values from -6 to 6
- kv_cache: bfloat16 [2, 1024, 16384], P(None, 'seq', ('groups', 'expert')), parts along dimension 2, may hold values from -6 to 6
- lengths: int32 [8], P('groups'), parts along dimension 0, may hold values from 128 to 2048, as said below
- routing: int32 [8, 2], P('groups'), parts along dimension 0, may hold values from 0 to 3, all different within a row
- w_out: bfloat16 [6144, 6144], P('expert', 'seq'), may hold values from -0.5 to 0.5
- norm_gain: bfloat16 [6144], replicated, may hold values from 0.5 to 1.5
- router: bfloat16 [6144, 4], replicated, may hold values from -0.078125 to 0.078125
- w_gate: bfloat16 [4, 6144, 1024], P('expert', None, 'seq'), may hold values from -0.078125 to 0.078125
- w_up: bfloat16 [4, 6144, 1024], P('expert', None, 'seq'), may hold values from -0.078125 to 0.078125
- w_down: bfloat16 [4, 1024, 6144], P('expert', 'seq'), may hold values from -0.75 to 0.75
Outputs:
- attended: bfloat16 [8, 6144], P('groups', 'seq'), parts along dimension 0
- expert_out: bfloat16 [8, 6144], P('groups', 'seq'), parts along dimension 0
The draws below stay inside these ranges and needn't reach their ends.
There are 2 independent parts, one for each index of `groups`. The reference program is written for one: setup_inputs(seed, part) draws one part's arguments, and reference() takes and returns one part's arrays. A program takes and returns all parts, laid end to end along the dimension named above; an argument that names none is the same for every part. Nothing has to cross between parts.
Inputs may be any that keep to these rules, and one draw needn't show every extreme that they name: `lengths`: every draw has a request of exactly 2048 positions. `routing`: each request names two different experts.
All inputs are finite; a program needn't handle non-finite values.
Results may differ from the reference program's by a relative error of at most 0.02.
Values may be sent and summed in bfloat16 or wider, within the bound.
A program may use at most 128 MiB of HBM per device.

```python
import math
import jax
import jax.numpy as jnp
from jax import lax

D = 6144
H = 48
KVH = 8
HD = 128
EXPERTS = 4
FF = 1024
REQ = 4
CTX = 2048


def draw_residual(key, part):
    drawn = 0.5 * jnp.clip(jax.random.normal(jax.random.fold_in(key, 1), (REQ, D), jnp.float32), -6.0, 6.0)
    return drawn.astype(jnp.bfloat16)


def draw_queries(key, part):
    drawn = jnp.clip(jax.random.normal(jax.random.fold_in(key, 4), (REQ, H * HD), jnp.float32), -6.0, 6.0)
    return drawn.astype(jnp.bfloat16)


def draw_new_entries(key, part):
    drawn = jnp.clip(jax.random.normal(jax.random.fold_in(key, 5), (2, REQ, KVH * HD), jnp.float32), -6.0, 6.0)
    return drawn.astype(jnp.bfloat16)


def draw_kv_cache(key, part):
    drawn = jnp.clip(jax.random.normal(jax.random.fold_in(key, 6), (2, KVH * HD, CTX * REQ), jnp.float32), -6.0, 6.0)
    return drawn.astype(jnp.bfloat16)


def draw_lengths(key, part):
    drawn = jax.random.randint(jax.random.fold_in(key, 11), (REQ,), CTX // 16, CTX + 1, dtype=jnp.int32)
    longest = jax.random.randint(jax.random.fold_in(key, 12), (), 0, REQ, dtype=jnp.int32)
    return jnp.where(jnp.arange(REQ, dtype=jnp.int32) == longest, CTX, drawn).astype(jnp.int32)


def spiked(values, key, source, target, shards_of, factor):
    def block_of(position):
        return (jnp.arange(values.shape[position]) // (values.shape[position] // shards_of)).reshape((-1,) + (1,) * (values.ndim - 1 - position))

    first = jax.random.permutation(key, shards_of)[block_of(target)]
    other_side = (block_of(target) + shards_of // 2) % shards_of
    return jnp.where((block_of(source) == first) | (block_of(source) == other_side), factor * values, values)


def block_levels(key, dims, split, least, largest):
    loudness = 1.0
    for position, parts in split:
        steps = jax.random.uniform(jax.random.fold_in(jax.random.fold_in(key, 6), position), (parts,), jnp.float32, least / len(split), largest / len(split))
        loudness = loudness * jnp.repeat(jnp.exp(steps), dims[position] // parts).reshape((-1,) + (1,) * (len(dims) - 1 - position))
    return loudness


def picks_of(own_key, rows, count, top, lift):
    ranking = jax.random.permutation(jax.random.fold_in(own_key, 1), count)
    pull = ranking
    for power in range(3):
        pull = pull * pull // count
    pull = pull * lift // count
    chance = jax.random.randint(jax.random.fold_in(own_key, 2), (rows, count), 0, 4096) + pull
    fixed_rows = jax.random.permutation(jax.random.fold_in(own_key, 3), rows)[jnp.arange(count) % rows]
    chance = jnp.where(jnp.arange(rows)[:, None] == fixed_rows[None, :], 1 << 14, chance)
    score = chance * count + jnp.arange(count)
    return lax.top_k(score.astype(jnp.int32), top)[1].astype(jnp.int32)


def gaussian(stream_key, shape, width, most, cuts=(), kind=jnp.bfloat16):
    values = width * jax.random.normal(stream_key, shape, jnp.float32)
    if cuts:
        values = values * block_levels(stream_key, shape, cuts, -0.22, 0.18)
    return jnp.clip(values, -most, most).astype(kind)


def gaussian_with(rng, extent, width, most, pieces, heavy, held_as=jnp.bfloat16):
    values = width * jax.random.normal(rng, extent, jnp.float32)
    if pieces:
        values = values * block_levels(rng, extent, pieces, -0.22, 0.18)
    return jnp.clip(spiked(values, jax.random.fold_in(rng, 3), *heavy), -most, most).astype(held_as)


def setup_inputs(seed: int = 0, part: int = 0) -> dict:
    seeds = jax.random.split(jax.random.key(seed), 13)
    part_keys = jax.random.split(jax.random.fold_in(seeds[12], part), 13)
    return {
        "residual": draw_residual(jax.random.fold_in(jax.random.fold_in(seeds[12], part), 71), part),
        "queries": draw_queries(jax.random.fold_in(jax.random.fold_in(seeds[12], part), 71), part),
        "new_entries": draw_new_entries(jax.random.fold_in(jax.random.fold_in(seeds[12], part), 71), part),
        "kv_cache": draw_kv_cache(jax.random.fold_in(jax.random.fold_in(seeds[12], part), 71), part),
        "lengths": draw_lengths(jax.random.fold_in(jax.random.fold_in(seeds[12], part), 71), part),
        "routing": picks_of(part_keys[5], REQ, EXPERTS, 2, 4096),
        "w_out": gaussian(seeds[6], (H * HD, D), HD ** -0.5, 0.5, ((0, 2), (1, 8))),
        "norm_gain": jnp.clip(1.0 + 0.1 * jax.random.normal(seeds[7], (D,), jnp.float32), 0.5, 1.5).astype(jnp.bfloat16),
        "router": gaussian(seeds[8], (D, EXPERTS), D ** -0.5, 0.078125),
        "w_gate": gaussian(seeds[9], (EXPERTS, D, FF), D ** -0.5, 0.078125, ((0, 2), (2, 8))),
        "w_up": gaussian(seeds[10], (EXPERTS, D, FF), D ** -0.5, 0.078125, ((0, 2), (2, 8))),
        "w_down": gaussian_with(seeds[11], (EXPERTS, FF, D), (FF // 8) ** -0.5, 0.75, ((0, 2), (1, 8)), (1, 2, 8, 2.0)),
    }


def reference(residual, queries, new_entries, kv_cache, lengths, routing, w_out, norm_gain, router, w_gate, w_up, w_down):
    per_group = H // KVH
    score_scale = 1.0 / math.sqrt(HD)
    key_rows = kv_cache[0].reshape(KVH, HD, CTX, REQ).astype(jnp.float32)
    value_rows = kv_cache[1].reshape(KVH, HD, CTX, REQ).astype(jnp.float32)
    query_heads = queries.reshape(REQ, KVH, per_group, HD).astype(jnp.float32)
    new_keys = new_entries[0].reshape(REQ, KVH, HD).astype(jnp.float32)
    new_values = new_entries[1].reshape(REQ, KVH, HD).astype(jnp.float32)
    scores = jnp.einsum('rgtd,gdpr->rgtp', query_heads, key_rows, precision=lax.Precision.HIGHEST) * score_scale
    own_score = jnp.einsum('rgtd,rgd->rgt', query_heads, new_keys, precision=lax.Precision.HIGHEST) * score_scale
    alive_mask = (jnp.arange(CTX, dtype=jnp.int32)[None, :] < lengths[:, None])[:, None, None, :]
    highest = jnp.maximum(lax.optimization_barrier(jnp.max(jnp.where(alive_mask, scores, -1e+30), axis=-1)), own_score)
    weights = jnp.where(alive_mask, jnp.exp(scores - highest[..., None]), 0.0)
    own_weight = jnp.exp(own_score - highest)
    totals = lax.optimization_barrier(jnp.sum(weights, axis=-1)) + own_weight
    rounded = lax.optimization_barrier(weights.astype(jnp.bfloat16)).astype(jnp.float32)
    summed = jnp.einsum('rgtp,gdpr->rgtd', rounded, value_rows, precision=lax.Precision.HIGHEST)
    summed = summed + own_weight[..., None] * new_values[:, :, None, :]
    attn_rows = (summed / totals[..., None]).reshape(REQ, H * HD).astype(jnp.bfloat16)
    attended = (residual.astype(jnp.float32) + jnp.dot(attn_rows, w_out, preferred_element_type=jnp.float32)).astype(jnp.bfloat16)
    widened = attended.astype(jnp.float32)
    mean_square = lax.optimization_barrier(jnp.mean(widened * widened, axis=-1, keepdims=True))
    normed = (widened * lax.rsqrt(mean_square + 1e-05) * norm_gain.astype(jnp.float32)).astype(jnp.bfloat16)
    logits = jnp.dot(normed, router, preferred_element_type=jnp.float32)
    picked = (routing[:, :, None] == jnp.arange(EXPERTS, dtype=jnp.int32)[None, None, :]).astype(jnp.float32)
    chosen = lax.optimization_barrier(jnp.sum(picked * logits[:, None, :], axis=-1))
    first_share = jax.nn.sigmoid(chosen[:, 0] - chosen[:, 1])
    shares = jnp.stack([first_share, 1.0 - first_share], axis=-1)
    combine = lax.optimization_barrier(jnp.sum(picked * shares[:, :, None], axis=1))

    def one_expert(expert):
        gate_proj = jnp.dot(normed, w_gate[expert], preferred_element_type=jnp.float32)
        upward = jnp.dot(normed, w_up[expert], preferred_element_type=jnp.float32)
        weight_col = lax.dynamic_slice_in_dim(combine, expert, 1, 1)
        activation = (jax.nn.silu(gate_proj) * upward * weight_col).astype(jnp.bfloat16)
        return jnp.dot(activation, w_down[expert], preferred_element_type=jnp.float32)
    expert_terms = lax.map(one_expert, jnp.arange(EXPERTS, dtype=jnp.int32))
    expert_out = lax.optimization_barrier(jnp.sum(expert_terms, axis=0)).astype(jnp.bfloat16)
    return (attended, expert_out)
```

```python
import functools
import math

import jax
import jax.numpy as jnp
from jax import lax
from jax.experimental import pallas as pl
from jax.experimental.pallas import tpu as pltpu
from jax.sharding import PartitionSpec as P

H = 48
KVH = 8
HD = 128


def combined_all(value, axis, join):
    pieces = jax.tree.map(lambda part: lax.all_gather(part, axis), value)
    head = jax.tree.map(lambda part: part[0], pieces)
    tail = jax.tree.map(lambda part: part[1:], pieces)
    running, _ = lax.scan(lambda running, share: (join(running, share), None), head, tail)
    return running


def merge_parts(earlier, later):
    high_left, total_left, sum_left = earlier
    high_right, total_right, sum_right = later
    joined = jnp.maximum(high_left, high_right)
    scale_left = jnp.exp(high_left - joined)
    scale_right = jnp.exp(high_right - joined)
    return (
        joined,
        total_left * scale_left + total_right * scale_right,
        sum_left * scale_left[..., None] + sum_right * scale_right[..., None],
    )


def partial_attention(query_rows, relaid, positions, lengths, kv_count):
    requests = lengths.shape[0]
    per_group = H // KVH
    slot_count = relaid.shape[2] // requests
    query_heads = query_rows.reshape(requests, kv_count, per_group, HD)
    key_rows = relaid[0].reshape(kv_count, HD, slot_count, requests)
    value_rows = relaid[1].reshape(kv_count, HD, slot_count, requests)
    scores = jnp.einsum(
        "rgtd,gdpr->rgtp", query_heads, key_rows, preferred_element_type=jnp.float32
    ) * (1.0 / math.sqrt(HD))
    alive_mask = (positions[None, :] < lengths[:, None])[:, None, None, :]
    highest = jnp.max(jnp.where(alive_mask, scores, -1e30), axis=-1)
    weights = jnp.where(alive_mask, jnp.exp(scores - highest[..., None]), 0.0)
    summed = jnp.einsum(
        "rgtp,gdpr->rgtd",
        weights.astype(jnp.bfloat16),
        value_rows,
        preferred_element_type=jnp.float32,
    )
    return (highest, jnp.sum(weights, axis=-1), summed)


def on_device(
    residual,
    queries,
    new_entries,
    kv_cache,
    lengths,
    routing,
    w_out,
    norm_gain,
    router,
    w_gate,
    w_up,
    w_down,
):
    requests = lengths.shape[0]
    seq_count = lax.axis_size("seq")
    core_count = lax.axis_size("expert")
    seq_index = lax.axis_index("seq")
    core_index = lax.axis_index("expert")
    half_ctx = kv_cache.shape[2] // requests
    ctx_dev = half_ctx // seq_count
    own_heads = KVH // core_count
    relaid = lax.all_to_all(kv_cache, "seq", split_axis=2, concat_axis=1, tiled=True)
    positions = core_index * half_ctx + seq_index * ctx_dev + jnp.arange(ctx_dev, dtype=jnp.int32)
    all_queries = lax.all_gather(queries, "expert", axis=1, tiled=True)
    partials = partial_attention(all_queries, relaid, positions, lengths, KVH)
    merged = combined_all(partials, ("seq", "expert"), merge_parts)
    head_start = core_index * own_heads
    highest = lax.dynamic_slice_in_dim(merged[0], head_start, own_heads, 1)
    totals = lax.dynamic_slice_in_dim(merged[1], head_start, own_heads, 1)
    summed = lax.dynamic_slice_in_dim(merged[2], head_start, own_heads, 1)
    per_group = H // KVH
    query_heads = queries.reshape(requests, own_heads, per_group, HD)
    new_keys = new_entries[0].reshape(requests, own_heads, HD)
    new_values = new_entries[1].reshape(requests, own_heads, HD).astype(jnp.float32)
    own_score = jnp.einsum(
        "rgtd,rgd->rgt", query_heads, new_keys, preferred_element_type=jnp.float32
    ) * (1.0 / math.sqrt(HD))
    joined = jnp.maximum(highest, own_score)
    fade_old = jnp.exp(highest - joined)
    own_weight = jnp.exp(own_score - joined)
    numerator = summed * fade_old[..., None] + own_weight[..., None] * new_values[:, :, None, :]
    denominator = totals * fade_old + own_weight
    attn_rows = (
        (numerator / denominator[..., None])
        .reshape(requests, own_heads * per_group * HD)
        .astype(jnp.bfloat16)
    )
    head_terms = jnp.dot(attn_rows, w_out, preferred_element_type=jnp.float32)
    attended = (residual.astype(jnp.float32) + lax.psum(head_terms, "expert")).astype(jnp.bfloat16)
    gathered = lax.all_gather(attended, "seq", axis=1, tiled=True)
    widened = gathered.astype(jnp.float32)
    mean_square = jnp.mean(widened * widened, axis=-1, keepdims=True)
    normed = (widened * lax.rsqrt(mean_square + 1e-05) * norm_gain.astype(jnp.float32)).astype(
        jnp.bfloat16
    )
    logits = jnp.dot(normed, router, preferred_element_type=jnp.float32)
    expert_total = router.shape[1]
    picked = (
        routing[:, :, None] == jnp.arange(expert_total, dtype=jnp.int32)[None, None, :]
    ).astype(jnp.float32)
    chosen = jnp.sum(picked * logits[:, None, :], axis=-1)
    first_share = jax.nn.sigmoid(chosen[:, 0] - chosen[:, 1])
    shares = jnp.stack([first_share, 1.0 - first_share], axis=-1)
    combine = jnp.sum(picked * shares[:, :, None], axis=1)
    local_ids = core_index * w_gate.shape[0] + jnp.arange(w_gate.shape[0], dtype=jnp.int32)
    select = (jnp.arange(expert_total, dtype=jnp.int32)[:, None] == local_ids[None, :]).astype(
        jnp.float32
    )
    local_share = jnp.sum(combine[:, :, None] * select[None, :, :], axis=1)
    gate_proj = jnp.einsum("rd,edf->ref", normed, w_gate, preferred_element_type=jnp.float32)
    upward = jnp.einsum("rd,edf->ref", normed, w_up, preferred_element_type=jnp.float32)
    activation = (jax.nn.silu(gate_proj) * upward * local_share[:, :, None]).astype(jnp.bfloat16)
    expert_terms = jnp.einsum("ref,efd->rd", activation, w_down, preferred_element_type=jnp.float32)
    reduced = lax.psum_scatter(expert_terms, "seq", scatter_dimension=1, tiled=True)
    expert_out = lax.psum(reduced, "expert").astype(jnp.bfloat16)
    return (attended, expert_out)


def fused_kernel(
    seq_count,
    lengths,
    routing,
    residual,
    queries,
    new_entries,
    kv_cache,
    w_out,
    gain,
    router,
    w_gate,
    w_up,
    w_down,
    attended_out,
    expert_out,
    k_buf,
    v_buf,
    wo_buf,
    gu_buf,
    wd_buf,
    router_buf,
    gain_buf,
    res_buf,
    new_buf,
    q_buf,
    q_rows,
    kn_rows,
    vn_rows,
    part_mine,
    part_other,
    attn_rows,
    attn_buf,
    proj_mine,
    proj_other,
    att_buf,
    red_send,
    red_buf,
    load_sems,
    q_sems,
    part_sems,
    attn_send,
    attn_recv,
    proj_sems,
    att_send,
    att_recv,
    down_send,
    down_recv,
):
    s = lax.axis_index("seq")
    c = lax.axis_index("expert")
    requests, width = residual.shape
    per_group = H // KVH
    rows = requests * per_group
    columns = kv_cache.shape[2]
    own_heads = KVH // 2
    experts, features, hidden = w_gate.shape
    owner_core = s // own_heads
    slot = lax.rem(s, own_heads)
    is_owner = c == owner_core
    other = {"expert": 1 - c}
    remote = functools.partial(
        pltpu.make_async_remote_copy, device_id_type=pl.DeviceIdType.MESH
    )

    head_span = per_group * HD
    q_cols = pl.ds(pl.multiple_of(slot * head_span, HD), head_span)
    n_cols = pl.ds(pl.multiple_of(slot * HD, HD), HD)
    load_q = pltpu.make_async_copy(queries.at[:, q_cols], q_buf, load_sems.at[0])
    load_new = pltpu.make_async_copy(new_entries.at[:, :, n_cols], new_buf, load_sems.at[1])
    load_k = pltpu.make_async_copy(kv_cache.at[0], k_buf, load_sems.at[2])
    load_v = pltpu.make_async_copy(kv_cache.at[1], v_buf, load_sems.at[3])
    load_wo = [
        pltpu.make_async_copy(
            w_out.at[pl.ds(h * head_span, head_span)], wo_buf.at[h], load_sems.at[4 + h]
        )
        for h in range(own_heads)
    ]
    at = 4 + own_heads
    load_res = pltpu.make_async_copy(residual, res_buf, load_sems.at[at])
    load_gain = pltpu.make_async_copy(gain, gain_buf, load_sems.at[at + 1])
    load_router = pltpu.make_async_copy(router, router_buf, load_sems.at[at + 2])
    load_gu = []
    load_wd = []
    for e in range(experts):
        for i, w in enumerate((w_gate, w_up)):
            load_gu.append(
                pltpu.make_async_copy(
                    w.at[e],
                    gu_buf.at[:, pl.ds((2 * e + i) * hidden, hidden)],
                    load_sems.at[at + 3],
                )
            )
        load_wd.append(
            pltpu.make_async_copy(
                w_down.at[e], wd_buf.at[pl.ds(e * hidden, hidden)], load_sems.at[at + 4]
            )
        )

    @pl.when(is_owner)
    def _():
        load_q.start()
        load_new.start()

    load_k.start()
    load_v.start()
    for load in load_wo:
        load.start()
    load_res.start()
    load_gain.start()
    load_router.start()
    for load in load_gu + load_wd:
        load.start()

    barrier = pltpu.get_barrier_semaphore()
    pl.semaphore_signal(barrier, inc=1, device_id=other, device_id_type=pl.DeviceIdType.MESH)
    for step in range(1, seq_count):
        peer = lax.rem(s + step, seq_count)
        for core in range(2):
            pl.semaphore_signal(
                barrier,
                inc=1,
                device_id={"seq": peer, "expert": core},
                device_id_type=pl.DeviceIdType.MESH,
            )
    pl.semaphore_wait(barrier, 2 * seq_count - 1)

    send_q = remote(
        src_ref=queries.at[:, q_cols],
        dst_ref=q_buf,
        send_sem=q_sems.at[0],
        recv_sem=q_sems.at[1],
        device_id=other,
    )

    @pl.when(is_owner)
    def _():
        send_q.start()
        load_q.wait()
        load_new.wait()

    @pl.when(jnp.logical_not(is_owner))
    def _():
        send_q.wait_recv()

    for t in range(per_group):
        q_rows[pl.ds(t * requests, requests), :] = q_buf[:, pl.ds(t * HD, HD)].astype(jnp.float32)
    q_f32 = q_rows[...]
    scale = 1.0 / math.sqrt(HD)
    load_k.wait()
    scores = (
        jnp.dot(q_f32.astype(jnp.bfloat16), k_buf[...], preferred_element_type=jnp.float32) * scale
    )
    row_id = lax.broadcasted_iota(jnp.int32, (rows, 1), 0)
    row_req = lax.rem(row_id, requests)
    limit = jnp.zeros((rows, 1), jnp.int32)
    for r in range(requests):
        limit = jnp.where(row_req == r, lengths[r], limit)
    limit = limit * requests - c * columns
    col_id = lax.broadcasted_iota(jnp.int32, (rows, columns), 1)
    alive = ((col_id & (requests - 1)) == row_req) & (col_id < limit)
    scores = jnp.where(alive, scores, -1e30)
    highest = jnp.max(scores, axis=-1, keepdims=True)
    weights = jnp.where(alive, jnp.exp(scores - highest), 0.0)
    total = jnp.sum(weights, axis=-1, keepdims=True)
    load_v.wait()
    summed = lax.dot_general(
        weights.astype(jnp.bfloat16),
        v_buf[...],
        (((1,), (1,)), ((), ())),
        preferred_element_type=jnp.float32,
    )

    send_part = remote(
        src_ref=part_mine,
        dst_ref=part_other,
        send_sem=part_sems.at[0],
        recv_sem=part_sems.at[1],
        device_id=other,
    )
    attn_copies = []
    for step in range(1, seq_count):
        peer = lax.rem(s + step, seq_count)
        attn_copies.append(
            remote(
                src_ref=attn_buf.at[slot],
                dst_ref=attn_buf.at[slot],
                send_sem=attn_send,
                recv_sem=attn_recv.at[slot],
                device_id={"seq": peer},
            )
        )

    lane = lax.broadcasted_iota(jnp.int32, (rows, HD), 1)

    @pl.when(jnp.logical_not(is_owner))
    def _():
        part_mine[0] = summed
        part_mine[1] = jnp.where(lane < HD // 2, highest, total)
        send_part.start()

    @pl.when(is_owner)
    def _():
        for t in range(per_group):
            kn_rows[pl.ds(t * requests, requests), :] = new_buf[0].astype(jnp.float32)
            vn_rows[pl.ds(t * requests, requests), :] = new_buf[1].astype(jnp.float32)
        own = jnp.sum(q_f32 * kn_rows[...], axis=-1, keepdims=True) * scale
        mine = jnp.maximum(highest, own)
        send_part.wait_recv()
        stats = part_other[1]
        high_other = stats[:, 0:1]
        total_other = stats[:, HD - 1 : HD]
        joined = jnp.maximum(mine, high_other)
        fade = jnp.exp(highest - joined)
        fade_other = jnp.exp(high_other - joined)
        own_weight = jnp.exp(own - joined)
        numer = summed * fade + part_other[0] * fade_other + own_weight * vn_rows[...]
        denom = total * fade + total_other * fade_other + own_weight
        attn_rows[...] = numer / denom
        for t in range(per_group):
            attn_buf[slot, :, pl.ds(t * HD, HD)] = attn_rows[
                pl.ds(t * requests, requests), :
            ].astype(jnp.bfloat16)
        for copy in attn_copies:
            copy.start()

    proj = jnp.zeros((requests, width), jnp.float32)
    for h in range(own_heads):
        load_wo[h].wait()

        @pl.when(jnp.logical_not(is_owner & (slot == h)))
        def _():
            remote(
                src_ref=attn_buf.at[h],
                dst_ref=attn_buf.at[h],
                send_sem=attn_send,
                recv_sem=attn_recv.at[h],
                device_id=other,
            ).wait_recv()

        proj = proj + jnp.dot(attn_buf[h], wo_buf[h], preferred_element_type=jnp.float32)
    proj_mine[...] = proj
    send_proj = remote(
        src_ref=proj_mine,
        dst_ref=proj_other,
        send_sem=proj_sems.at[0],
        recv_sem=proj_sems.at[1],
        device_id=other,
    )
    send_proj.start()
    load_res.wait()
    load_gain.wait()
    load_router.wait()
    for load in load_gu:
        load.wait()
    res_f32 = res_buf[...].astype(jnp.float32)
    send_proj.wait_recv()
    attended = (res_f32 + (proj + proj_other[...])).astype(jnp.bfloat16)
    att_buf[s] = attended
    attended_out[...] = attended
    att_copies = []
    for step in range(1, seq_count):
        peer = lax.rem(s + step, seq_count)
        att_copies.append(
            remote(
                src_ref=att_buf.at[s],
                dst_ref=att_buf.at[s],
                send_sem=att_send,
                recv_sem=att_recv.at[s],
                device_id={"seq": peer},
            )
        )
    for copy in att_copies:
        copy.start()

    squares = jnp.zeros((requests, 1), jnp.float32)
    logits = jnp.zeros((requests, router.shape[0]), jnp.float32)
    gu = jnp.zeros((requests, 2 * experts * hidden), jnp.float32)
    for i in range(seq_count):

        @pl.when(s != i)
        def _():
            remote(
                src_ref=att_buf.at[i],
                dst_ref=att_buf.at[i],
                send_sem=att_send,
                recv_sem=att_recv.at[i],
                device_id=other,
            ).wait_recv()

        x = att_buf[i].astype(jnp.float32)
        squares = squares + jnp.sum(x * x, axis=-1, keepdims=True)
        scaled = (x * gain_buf[:, pl.ds(i * width, width)]).astype(jnp.bfloat16)
        logits = logits + lax.dot_general(
            scaled,
            router_buf[:, pl.ds(i * width, width)],
            (((1,), (1,)), ((), ())),
            preferred_element_type=jnp.float32,
        )
        gu = gu + jnp.dot(
            scaled, gu_buf[pl.ds(i * width, width), :], preferred_element_type=jnp.float32
        )
    inverse = lax.rsqrt(squares * (1.0 / features) + 1e-05)
    logits = logits * inverse
    gu = gu * inverse
    req_id = lax.broadcasted_iota(jnp.int32, (requests, 1), 0)
    first_id = jnp.zeros((requests, 1), jnp.int32)
    second_id = jnp.zeros((requests, 1), jnp.int32)
    for r in range(requests):
        first_id = jnp.where(req_id == r, routing[0, r], first_id)
        second_id = jnp.where(req_id == r, routing[1, r], second_id)
    expert_id = lax.broadcasted_iota(jnp.int32, logits.shape, 1)
    gap = jnp.sum(
        jnp.where(expert_id == first_id, logits, 0.0)
        - jnp.where(expert_id == second_id, logits, 0.0),
        axis=-1,
        keepdims=True,
    )
    first_share = 1.0 / (1.0 + jnp.exp(-gap))
    acts = []
    for e in range(experts):
        number = c * experts + e
        share = jnp.where(number == first_id, first_share, 0.0) + jnp.where(
            number == second_id, 1.0 - first_share, 0.0
        )
        gate = gu[:, 2 * e * hidden : (2 * e + 1) * hidden]
        up = gu[:, (2 * e + 1) * hidden : (2 * e + 2) * hidden]
        acts.append((gate / (1.0 + jnp.exp(-gate)) * up * share).astype(jnp.bfloat16))
    act = jnp.concatenate(acts, axis=1)
    for load in load_wd:
        load.wait()

    me = s * 2 + c
    down_copies = []
    for step in range(1, seq_count + 1):
        peer = lax.rem(s + step, seq_count)
        block = jnp.dot(
            act,
            wd_buf[:, pl.ds(pl.multiple_of(peer * width, HD), width)],
            preferred_element_type=jnp.float32,
        ).astype(jnp.bfloat16)
        if step < seq_count:
            red_send[step - 1] = block
            for core in range(2):
                copy = remote(
                    src_ref=red_send.at[step - 1],
                    dst_ref=red_buf.at[me],
                    send_sem=down_send,
                    recv_sem=down_recv.at[me],
                    device_id={"seq": peer, "expert": core},
                )
                copy.start()
                down_copies.append(copy)
        else:
            red_buf[me] = block
            copy = remote(
                src_ref=red_buf.at[me],
                dst_ref=red_buf.at[me],
                send_sem=down_send,
                recv_sem=down_recv.at[me],
                device_id=other,
            )
            copy.start()
            down_copies.append(copy)
    result = jnp.zeros((requests, width), jnp.float32)
    for i in range(2 * seq_count):

        @pl.when(me != i)
        def _():
            remote(
                src_ref=red_buf.at[i],
                dst_ref=red_buf.at[i],
                send_sem=down_send,
                recv_sem=down_recv.at[i],
                device_id=other,
            ).wait_recv()

        result = result + red_buf[i].astype(jnp.float32)
    expert_out[...] = result.astype(jnp.bfloat16)

    @pl.when(is_owner)
    def _():
        send_q.wait_send()
        for copy in attn_copies:
            copy.wait_send()

    @pl.when(jnp.logical_not(is_owner))
    def _():
        send_part.wait_send()

    send_proj.wait_send()
    for copy in att_copies + down_copies:
        copy.wait_send()


def fused_step(
    residual,
    queries,
    new_entries,
    kv_cache,
    lengths,
    routing,
    w_out,
    norm_gain,
    router,
    w_gate,
    w_up,
    w_down,
):
    seq_count = lax.axis_size("seq")
    requests, width = residual.shape
    per_group = H // KVH
    own_heads = KVH // 2
    rows = requests * per_group
    columns = kv_cache.shape[2]
    experts, features, hidden = w_gate.shape
    gain = norm_gain.astype(jnp.float32).reshape(1, features)
    bf16, f32 = jnp.bfloat16, jnp.float32
    vmem = pltpu.VMEM
    dma = pltpu.SemaphoreType.DMA
    anywhere = pl.BlockSpec(memory_space=pl.ANY)
    out = jax.ShapeDtypeStruct((requests, width), bf16)
    return pl.pallas_call(
        functools.partial(fused_kernel, seq_count),
        out_shape=(out, out),
        in_specs=[pl.BlockSpec(memory_space=pltpu.SMEM)] * 2 + [anywhere] * 10,
        out_specs=(pl.BlockSpec(memory_space=vmem),) * 2,
        scratch_shapes=[
            vmem((HD, columns), bf16),
            vmem((HD, columns), bf16),
            vmem((own_heads, per_group * HD, width), bf16),
            vmem((features, 2 * experts * hidden), bf16),
            vmem((experts * hidden, features), bf16),
            vmem((router.shape[1], features), bf16),
            vmem((1, features), f32),
            vmem((requests, width), bf16),
            vmem((2, requests, HD), bf16),
            vmem((requests, per_group * HD), bf16),
            vmem((rows, HD), f32),
            vmem((rows, HD), f32),
            vmem((rows, HD), f32),
            vmem((2, rows, HD), f32),
            vmem((2, rows, HD), f32),
            vmem((rows, HD), f32),
            vmem((own_heads, requests, per_group * HD), bf16),
            vmem((requests, width), f32),
            vmem((requests, width), f32),
            vmem((seq_count, requests, width), bf16),
            vmem((seq_count, requests, width), bf16),
            vmem((2 * seq_count, requests, width), bf16),
            dma((9 + own_heads,)),
            dma((2,)),
            dma((2,)),
            dma,
            dma((own_heads,)),
            dma((2,)),
            dma,
            dma((seq_count,)),
            dma,
            dma((2 * seq_count,)),
        ],
        compiler_params=pltpu.CompilerParams(
            collective_id=0, has_side_effects=True, vmem_limit_bytes=60 * 1024 * 1024
        ),
        name="decode_step",
    )(
        lengths,
        routing.T,
        residual,
        queries,
        new_entries,
        kv_cache,
        w_out,
        gain,
        router.T,
        w_gate,
        w_up,
        w_down,
    )


def step_on_device(*args):
    kv_cache, lengths = args[3], args[4]
    requests = lengths.shape[0]
    whole_head = kv_cache.shape[1] == HD and lax.axis_size("seq") == KVH
    if whole_head and lax.axis_size("expert") == 2 and requests & (requests - 1) == 0:
        return fused_step(*args)
    return on_device(*args)


def solution(mesh):
    in_specs = (
        P("groups", "seq"),
        P("groups", "expert"),
        P(None, "groups", "expert"),
        P(None, "seq", ("groups", "expert")),
        P("groups"),
        P("groups", None),
        P("expert", "seq"),
        P(),
        P(),
        P("expert", None, "seq"),
        P("expert", None, "seq"),
        P("expert", "seq", None),
    )
    out_specs = (P("groups", "seq"), P("groups", "seq"))
    return jax.shard_map(
        step_on_device, mesh=mesh, in_specs=in_specs, out_specs=out_specs, check_vma=False
    )
```

```python
import functools
import math

import jax
import jax.numpy as jnp
from jax import lax
from jax.experimental import pallas as pl
from jax.experimental.pallas import tpu as pltpu
from jax.sharding import PartitionSpec as P

H = 48
KVH = 8
HD = 128


def combined_all(value, axis, join):
    pieces = jax.tree.map(lambda part: lax.all_gather(part, axis), value)
    head = jax.tree.map(lambda part: part[0], pieces)
    tail = jax.tree.map(lambda part: part[1:], pieces)
    running, _ = lax.scan(lambda running, share: (join(running, share), None), head, tail)
    return running


def merge_parts(earlier, later):
    high_left, total_left, sum_left = earlier
    high_right, total_right, sum_right = later
    joined = jnp.maximum(high_left, high_right)
    scale_left = jnp.exp(high_left - joined)
    scale_right = jnp.exp(high_right - joined)
    return (
        joined,
        total_left * scale_left + total_right * scale_right,
        sum_left * scale_left[..., None] + sum_right * scale_right[..., None],
    )


def partial_attention(query_rows, relaid, positions, lengths, kv_count):
    requests = lengths.shape[0]
    per_group = H // KVH
    slot_count = relaid.shape[2] // requests
    query_heads = query_rows.reshape(requests, kv_count, per_group, HD)
    key_rows = relaid[0].reshape(kv_count, HD, slot_count, requests)
    value_rows = relaid[1].reshape(kv_count, HD, slot_count, requests)
    scores = jnp.einsum(
        "rgtd,gdpr->rgtp", query_heads, key_rows, preferred_element_type=jnp.float32
    ) * (1.0 / math.sqrt(HD))
    alive_mask = (positions[None, :] < lengths[:, None])[:, None, None, :]
    highest = jnp.max(jnp.where(alive_mask, scores, -1e30), axis=-1)
    weights = jnp.where(alive_mask, jnp.exp(scores - highest[..., None]), 0.0)
    summed = jnp.einsum(
        "rgtp,gdpr->rgtd",
        weights.astype(jnp.bfloat16),
        value_rows,
        preferred_element_type=jnp.float32,
    )
    return (highest, jnp.sum(weights, axis=-1), summed)


def on_device(
    residual,
    queries,
    new_entries,
    kv_cache,
    lengths,
    routing,
    w_out,
    norm_gain,
    router,
    w_gate,
    w_up,
    w_down,
):
    requests = lengths.shape[0]
    seq_count = lax.axis_size("seq")
    core_count = lax.axis_size("expert")
    seq_index = lax.axis_index("seq")
    core_index = lax.axis_index("expert")
    half_ctx = kv_cache.shape[2] // requests
    ctx_dev = half_ctx // seq_count
    own_heads = KVH // core_count
    relaid = lax.all_to_all(kv_cache, "seq", split_axis=2, concat_axis=1, tiled=True)
    positions = core_index * half_ctx + seq_index * ctx_dev + jnp.arange(ctx_dev, dtype=jnp.int32)
    all_queries = lax.all_gather(queries, "expert", axis=1, tiled=True)
    partials = partial_attention(all_queries, relaid, positions, lengths, KVH)
    merged = combined_all(partials, ("seq", "expert"), merge_parts)
    head_start = core_index * own_heads
    highest = lax.dynamic_slice_in_dim(merged[0], head_start, own_heads, 1)
    totals = lax.dynamic_slice_in_dim(merged[1], head_start, own_heads, 1)
    summed = lax.dynamic_slice_in_dim(merged[2], head_start, own_heads, 1)
    per_group = H // KVH
    query_heads = queries.reshape(requests, own_heads, per_group, HD)
    new_keys = new_entries[0].reshape(requests, own_heads, HD)
    new_values = new_entries[1].reshape(requests, own_heads, HD).astype(jnp.float32)
    own_score = jnp.einsum(
        "rgtd,rgd->rgt", query_heads, new_keys, preferred_element_type=jnp.float32
    ) * (1.0 / math.sqrt(HD))
    joined = jnp.maximum(highest, own_score)
    fade_old = jnp.exp(highest - joined)
    own_weight = jnp.exp(own_score - joined)
    numerator = summed * fade_old[..., None] + own_weight[..., None] * new_values[:, :, None, :]
    denominator = totals * fade_old + own_weight
    attn_rows = (
        (numerator / denominator[..., None])
        .reshape(requests, own_heads * per_group * HD)
        .astype(jnp.bfloat16)
    )
    head_terms = jnp.dot(attn_rows, w_out, preferred_element_type=jnp.float32)
    attended = (residual.astype(jnp.float32) + lax.psum(head_terms, "expert")).astype(jnp.bfloat16)
    gathered = lax.all_gather(attended, "seq", axis=1, tiled=True)
    widened = gathered.astype(jnp.float32)
    mean_square = jnp.mean(widened * widened, axis=-1, keepdims=True)
    normed = (widened * lax.rsqrt(mean_square + 1e-05) * norm_gain.astype(jnp.float32)).astype(
        jnp.bfloat16
    )
    logits = jnp.dot(normed, router, preferred_element_type=jnp.float32)
    expert_total = router.shape[1]
    picked = (
        routing[:, :, None] == jnp.arange(expert_total, dtype=jnp.int32)[None, None, :]
    ).astype(jnp.float32)
    chosen = jnp.sum(picked * logits[:, None, :], axis=-1)
    first_share = jax.nn.sigmoid(chosen[:, 0] - chosen[:, 1])
    shares = jnp.stack([first_share, 1.0 - first_share], axis=-1)
    combine = jnp.sum(picked * shares[:, :, None], axis=1)
    local_ids = core_index * w_gate.shape[0] + jnp.arange(w_gate.shape[0], dtype=jnp.int32)
    select = (jnp.arange(expert_total, dtype=jnp.int32)[:, None] == local_ids[None, :]).astype(
        jnp.float32
    )
    local_share = jnp.sum(combine[:, :, None] * select[None, :, :], axis=1)
    gate_proj = jnp.einsum("rd,edf->ref", normed, w_gate, preferred_element_type=jnp.float32)
    upward = jnp.einsum("rd,edf->ref", normed, w_up, preferred_element_type=jnp.float32)
    activation = (jax.nn.silu(gate_proj) * upward * local_share[:, :, None]).astype(jnp.bfloat16)
    expert_terms = jnp.einsum("ref,efd->rd", activation, w_down, preferred_element_type=jnp.float32)
    reduced = lax.psum_scatter(expert_terms, "seq", scatter_dimension=1, tiled=True)
    expert_out = lax.psum(reduced, "expert").astype(jnp.bfloat16)
    return (attended, expert_out)


def fused_kernel(
    seq_count,
    lengths,
    routing,
    residual,
    queries,
    new_entries,
    kv_cache,
    w_out,
    gain,
    router,
    w_gate,
    w_up,
    w_down,
    outs,
    k_buf,
    v_buf,
    wo_buf,
    gu_buf,
    wd_buf,
    router_buf,
    gain_buf,
    res_buf,
    new_buf,
    q_buf,
    q_rows,
    kn_rows,
    vn_rows,
    part_mine,
    part_other,
    attn_rows,
    attn_buf,
    proj_mine,
    proj_other,
    att_buf,
    red_send,
    red_buf,
    load_sems,
    q_sems,
    part_sems,
    attn_send,
    attn_recv,
    proj_sems,
    att_send,
    att_recv,
    down_send,
    down_recv,
):
    s = lax.axis_index("seq")
    c = lax.axis_index("expert")
    requests, width = residual.shape
    per_group = H // KVH
    rows = requests * per_group
    columns = kv_cache.shape[2]
    own_heads = KVH // 2
    experts, features, hidden = w_gate.shape
    owner_core = s // own_heads
    slot = lax.rem(s, own_heads)
    is_owner = c == owner_core
    other = {"expert": 1 - c}
    remote = functools.partial(
        pltpu.make_async_remote_copy, device_id_type=pl.DeviceIdType.MESH
    )

    head_span = per_group * HD
    q_cols = pl.ds(pl.multiple_of(slot * head_span, HD), head_span)
    n_cols = pl.ds(pl.multiple_of(slot * HD, HD), HD)
    load_q = pltpu.make_async_copy(queries.at[:, q_cols], q_buf, load_sems.at[0])
    load_new = pltpu.make_async_copy(new_entries.at[:, :, n_cols], new_buf, load_sems.at[1])
    load_k = pltpu.make_async_copy(kv_cache.at[0], k_buf, load_sems.at[2])
    load_v = pltpu.make_async_copy(kv_cache.at[1], v_buf, load_sems.at[3])
    load_wo = [
        pltpu.make_async_copy(
            w_out.at[pl.ds(h * head_span, head_span)], wo_buf.at[h], load_sems.at[4 + h]
        )
        for h in range(own_heads)
    ]
    at = 4 + own_heads
    load_res = pltpu.make_async_copy(residual, res_buf, load_sems.at[at])
    load_gain = pltpu.make_async_copy(gain, gain_buf, load_sems.at[at + 1])
    load_router = pltpu.make_async_copy(router, router_buf, load_sems.at[at + 2])
    load_gu = []
    load_wd = []
    for e in range(experts):
        for i, w in enumerate((w_gate, w_up)):
            load_gu.append(
                pltpu.make_async_copy(
                    w.at[e],
                    gu_buf.at[:, pl.ds((2 * e + i) * hidden, hidden)],
                    load_sems.at[at + 3],
                )
            )
        load_wd.append(
            pltpu.make_async_copy(
                w_down.at[e], wd_buf.at[pl.ds(e * hidden, hidden)], load_sems.at[at + 4]
            )
        )

    @pl.when(is_owner)
    def _():
        load_q.start()
        load_new.start()

    load_k.start()
    load_v.start()
    for load in load_wo:
        load.start()
    load_res.start()
    load_gain.start()
    load_router.start()
    for load in load_gu + load_wd:
        load.start()

    barrier = pltpu.get_barrier_semaphore()
    pl.semaphore_signal(barrier, inc=1, device_id=other, device_id_type=pl.DeviceIdType.MESH)
    for step in range(1, seq_count):
        peer = lax.rem(s + step, seq_count)
        for core in range(2):
            pl.semaphore_signal(
                barrier,
                inc=1,
                device_id={"seq": peer, "expert": core},
                device_id_type=pl.DeviceIdType.MESH,
            )
    pl.semaphore_wait(barrier, 2 * seq_count - 1)

    send_q = remote(
        src_ref=queries.at[:, q_cols],
        dst_ref=q_buf,
        send_sem=q_sems.at[0],
        recv_sem=q_sems.at[1],
        device_id=other,
    )

    @pl.when(is_owner)
    def _():
        send_q.start()
        load_q.wait()
        load_new.wait()

    @pl.when(jnp.logical_not(is_owner))
    def _():
        send_q.wait_recv()

    for t in range(per_group):
        q_rows[pl.ds(t * requests, requests), :] = q_buf[:, pl.ds(t * HD, HD)].astype(jnp.float32)
    q_f32 = q_rows[...]
    scale = 1.0 / math.sqrt(HD)
    load_k.wait()
    scores = (
        jnp.dot(q_f32.astype(jnp.bfloat16), k_buf[...], preferred_element_type=jnp.float32) * scale
    )
    row_id = lax.broadcasted_iota(jnp.int32, (rows, 1), 0)
    row_req = lax.rem(row_id, requests)
    limit = jnp.zeros((rows, 1), jnp.int32)
    for r in range(requests):
        limit = jnp.where(row_req == r, lengths[r], limit)
    limit = limit * requests - c * columns
    col_id = lax.broadcasted_iota(jnp.int32, (rows, columns), 1)
    alive = ((col_id & (requests - 1)) == row_req) & (col_id < limit)
    scores = jnp.where(alive, scores, -1e30)
    highest = jnp.max(scores, axis=-1, keepdims=True)
    weights = jnp.where(alive, jnp.exp(scores - highest), 0.0)
    total = jnp.sum(weights, axis=-1, keepdims=True)
    load_v.wait()
    summed = lax.dot_general(
        weights.astype(jnp.bfloat16),
        v_buf[...],
        (((1,), (1,)), ((), ())),
        preferred_element_type=jnp.float32,
    )

    send_part = remote(
        src_ref=part_mine,
        dst_ref=part_other,
        send_sem=part_sems.at[0],
        recv_sem=part_sems.at[1],
        device_id=other,
    )
    attn_copies = []
    for step in range(1, seq_count):
        peer = lax.rem(s + step, seq_count)
        attn_copies.append(
            remote(
                src_ref=attn_buf.at[slot],
                dst_ref=attn_buf.at[slot],
                send_sem=attn_send,
                recv_sem=attn_recv.at[slot],
                device_id={"seq": peer},
            )
        )

    lane = lax.broadcasted_iota(jnp.int32, (rows, HD), 1)

    @pl.when(jnp.logical_not(is_owner))
    def _():
        part_mine[0] = summed
        part_mine[1] = jnp.where(lane < HD // 2, highest, total)
        send_part.start()

    @pl.when(is_owner)
    def _():
        for t in range(per_group):
            kn_rows[pl.ds(t * requests, requests), :] = new_buf[0].astype(jnp.float32)
            vn_rows[pl.ds(t * requests, requests), :] = new_buf[1].astype(jnp.float32)
        own = jnp.sum(q_f32 * kn_rows[...], axis=-1, keepdims=True) * scale
        mine = jnp.maximum(highest, own)
        send_part.wait_recv()
        stats = part_other[1]
        high_other = stats[:, 0:1]
        total_other = stats[:, HD - 1 : HD]
        joined = jnp.maximum(mine, high_other)
        fade = jnp.exp(highest - joined)
        fade_other = jnp.exp(high_other - joined)
        own_weight = jnp.exp(own - joined)
        numer = summed * fade + part_other[0] * fade_other + own_weight * vn_rows[...]
        denom = total * fade + total_other * fade_other + own_weight
        attn_rows[...] = numer / denom
        for t in range(per_group):
            attn_buf[slot, :, pl.ds(t * HD, HD)] = attn_rows[
                pl.ds(t * requests, requests), :
            ].astype(jnp.bfloat16)
        for copy in attn_copies:
            copy.start()

    proj = jnp.zeros((requests, width), jnp.float32)
    for h in range(own_heads):
        load_wo[h].wait()

        @pl.when(jnp.logical_not(is_owner & (slot == h)))
        def _():
            remote(
                src_ref=attn_buf.at[h],
                dst_ref=attn_buf.at[h],
                send_sem=attn_send,
                recv_sem=attn_recv.at[h],
                device_id=other,
            ).wait_recv()

        proj = proj + jnp.dot(attn_buf[h], wo_buf[h], preferred_element_type=jnp.float32)
    proj_mine[...] = proj
    send_proj = remote(
        src_ref=proj_mine,
        dst_ref=proj_other,
        send_sem=proj_sems.at[0],
        recv_sem=proj_sems.at[1],
        device_id=other,
    )
    send_proj.start()
    load_res.wait()
    load_gain.wait()
    load_router.wait()
    for load in load_gu:
        load.wait()
    res_f32 = res_buf[...].astype(jnp.float32)
    send_proj.wait_recv()
    attended = (res_f32 + (proj + proj_other[...])).astype(jnp.bfloat16)
    att_buf[s] = attended
    outs[0] = attended
    att_copies = []
    for step in range(1, seq_count):
        peer = lax.rem(s + step, seq_count)
        att_copies.append(
            remote(
                src_ref=att_buf.at[s],
                dst_ref=att_buf.at[s],
                send_sem=att_send,
                recv_sem=att_recv.at[s],
                device_id={"seq": peer},
            )
        )
    for copy in att_copies:
        copy.start()

    squares = jnp.zeros((requests, 1), jnp.float32)
    logits = jnp.zeros((requests, router.shape[0]), jnp.float32)
    gu = jnp.zeros((requests, 2 * experts * hidden), jnp.float32)
    for i in range(seq_count):

        @pl.when(s != i)
        def _():
            remote(
                src_ref=att_buf.at[i],
                dst_ref=att_buf.at[i],
                send_sem=att_send,
                recv_sem=att_recv.at[i],
                device_id=other,
            ).wait_recv()

        x = att_buf[i].astype(jnp.float32)
        squares = squares + jnp.sum(x * x, axis=-1, keepdims=True)
        scaled = (x * gain_buf[pl.ds(i * width, width)].astype(jnp.float32)[None, :]).astype(jnp.bfloat16)
        logits = logits + lax.dot_general(
            scaled,
            router_buf[:, pl.ds(i * width, width)],
            (((1,), (1,)), ((), ())),
            preferred_element_type=jnp.float32,
        )
        gu = gu + jnp.dot(
            scaled, gu_buf[pl.ds(i * width, width), :], preferred_element_type=jnp.float32
        )
    inverse = lax.rsqrt(squares * (1.0 / features) + 1e-05)
    logits = logits * inverse
    gu = gu * inverse
    req_id = lax.broadcasted_iota(jnp.int32, (requests, 1), 0)
    first_id = jnp.zeros((requests, 1), jnp.int32)
    second_id = jnp.zeros((requests, 1), jnp.int32)
    for r in range(requests):
        first_id = jnp.where(req_id == r, routing[0, r], first_id)
        second_id = jnp.where(req_id == r, routing[1, r], second_id)
    expert_id = lax.broadcasted_iota(jnp.int32, logits.shape, 1)
    gap = jnp.sum(
        jnp.where(expert_id == first_id, logits, 0.0)
        - jnp.where(expert_id == second_id, logits, 0.0),
        axis=-1,
        keepdims=True,
    )
    first_share = 1.0 / (1.0 + jnp.exp(-gap))
    acts = []
    for e in range(experts):
        number = c * experts + e
        share = jnp.where(number == first_id, first_share, 0.0) + jnp.where(
            number == second_id, 1.0 - first_share, 0.0
        )
        gate = gu[:, 2 * e * hidden : (2 * e + 1) * hidden]
        up = gu[:, (2 * e + 1) * hidden : (2 * e + 2) * hidden]
        acts.append((gate / (1.0 + jnp.exp(-gate)) * up * share).astype(jnp.bfloat16))
    act = jnp.concatenate(acts, axis=1)
    for load in load_wd:
        load.wait()

    me = s * 2 + c
    down_copies = []
    for step in range(1, seq_count + 1):
        peer = lax.rem(s + step, seq_count)
        block = jnp.dot(
            act,
            wd_buf[:, pl.ds(pl.multiple_of(peer * width, HD), width)],
            preferred_element_type=jnp.float32,
        ).astype(jnp.bfloat16)
        if step < seq_count:
            red_send[step - 1] = block
            for core in range(2):
                copy = remote(
                    src_ref=red_send.at[step - 1],
                    dst_ref=red_buf.at[me],
                    send_sem=down_send,
                    recv_sem=down_recv.at[me],
                    device_id={"seq": peer, "expert": core},
                )
                copy.start()
                down_copies.append(copy)
        else:
            red_buf[me] = block
            copy = remote(
                src_ref=red_buf.at[me],
                dst_ref=red_buf.at[me],
                send_sem=down_send,
                recv_sem=down_recv.at[me],
                device_id=other,
            )
            copy.start()
            down_copies.append(copy)
    result = jnp.zeros((requests, width), jnp.float32)
    for i in range(2 * seq_count):

        @pl.when(me != i)
        def _():
            remote(
                src_ref=red_buf.at[i],
                dst_ref=red_buf.at[i],
                send_sem=down_send,
                recv_sem=down_recv.at[i],
                device_id=other,
            ).wait_recv()

        result = result + red_buf[i].astype(jnp.float32)
    outs[1] = result.astype(jnp.bfloat16)

    @pl.when(is_owner)
    def _():
        send_q.wait_send()
        for copy in attn_copies:
            copy.wait_send()

    @pl.when(jnp.logical_not(is_owner))
    def _():
        send_part.wait_send()

    send_proj.wait_send()
    for copy in att_copies + down_copies:
        copy.wait_send()


def fused_step(
    residual,
    queries,
    new_entries,
    kv_cache,
    lengths,
    routing,
    w_out,
    norm_gain,
    router,
    w_gate,
    w_up,
    w_down,
):
    seq_count = lax.axis_size("seq")
    requests, width = residual.shape
    per_group = H // KVH
    own_heads = KVH // 2
    rows = requests * per_group
    columns = kv_cache.shape[2]
    experts, features, hidden = w_gate.shape
    bf16, f32 = jnp.bfloat16, jnp.float32
    vmem = pltpu.VMEM
    dma = pltpu.SemaphoreType.DMA
    anywhere = pl.BlockSpec(memory_space=pl.ANY)
    out = jax.ShapeDtypeStruct((2, requests, width), bf16)
    outs = pl.pallas_call(
        functools.partial(fused_kernel, seq_count),
        out_shape=out,
        in_specs=[pl.BlockSpec(memory_space=pltpu.SMEM)] * 2 + [anywhere] * 10,
        out_specs=pl.BlockSpec(memory_space=vmem),
        scratch_shapes=[
            vmem((HD, columns), bf16),
            vmem((HD, columns), bf16),
            vmem((own_heads, per_group * HD, width), bf16),
            vmem((features, 2 * experts * hidden), bf16),
            vmem((experts * hidden, features), bf16),
            vmem((router.shape[1], features), bf16),
            vmem((features,), bf16),
            vmem((requests, width), bf16),
            vmem((2, requests, HD), bf16),
            vmem((requests, per_group * HD), bf16),
            vmem((rows, HD), f32),
            vmem((rows, HD), f32),
            vmem((rows, HD), f32),
            vmem((2, rows, HD), f32),
            vmem((2, rows, HD), f32),
            vmem((rows, HD), f32),
            vmem((own_heads, requests, per_group * HD), bf16),
            vmem((requests, width), f32),
            vmem((requests, width), f32),
            vmem((seq_count, requests, width), bf16),
            vmem((seq_count, requests, width), bf16),
            vmem((2 * seq_count, requests, width), bf16),
            dma((9 + own_heads,)),
            dma((2,)),
            dma((2,)),
            dma,
            dma((own_heads,)),
            dma((2,)),
            dma,
            dma((seq_count,)),
            dma,
            dma((2 * seq_count,)),
        ],
        compiler_params=pltpu.CompilerParams(
            collective_id=0, has_side_effects=True, vmem_limit_bytes=60 * 1024 * 1024
        ),
        name="decode_step",
    )(
        lengths,
        routing.T,
        residual,
        queries,
        new_entries,
        kv_cache,
        w_out,
        norm_gain,
        router.T,
        w_gate,
        w_up,
        w_down,
    )
    return (outs[0], outs[1])


def step_on_device(*args):
    kv_cache, lengths = args[3], args[4]
    requests = lengths.shape[0]
    whole_head = kv_cache.shape[1] == HD and lax.axis_size("seq") == KVH
    if whole_head and lax.axis_size("expert") == 2 and requests & (requests - 1) == 0:
        return fused_step(*args)
    return on_device(*args)


def solution(mesh):
    in_specs = (
        P("groups", "seq"),
        P("groups", "expert"),
        P(None, "groups", "expert"),
        P(None, "seq", ("groups", "expert")),
        P("groups"),
        P("groups", None),
        P("expert", "seq"),
        P(),
        P(),
        P("expert", None, "seq"),
        P("expert", None, "seq"),
        P("expert", "seq", None),
    )
    out_specs = (P("groups", "seq"), P("groups", "seq"))
    return jax.shard_map(
        step_on_device, mesh=mesh, in_specs=in_specs, out_specs=out_specs, check_vma=False
    )
```

```python
import functools
import math

import jax
import jax.numpy as jnp
from jax import lax
from jax.experimental import pallas as pl
from jax.experimental.pallas import tpu as pltpu
from jax.sharding import PartitionSpec as P

H = 48
KVH = 8
HD = 128


def combined_all(value, axis, join):
    pieces = jax.tree.map(lambda part: lax.all_gather(part, axis), value)
    head = jax.tree.map(lambda part: part[0], pieces)
    tail = jax.tree.map(lambda part: part[1:], pieces)
    running, _ = lax.scan(lambda running, share: (join(running, share), None), head, tail)
    return running


def merge_parts(earlier, later):
    high_left, total_left, sum_left = earlier
    high_right, total_right, sum_right = later
    joined = jnp.maximum(high_left, high_right)
    scale_left = jnp.exp(high_left - joined)
    scale_right = jnp.exp(high_right - joined)
    return (
        joined,
        total_left * scale_left + total_right * scale_right,
        sum_left * scale_left[..., None] + sum_right * scale_right[..., None],
    )


def partial_attention(query_rows, relaid, positions, lengths, kv_count):
    requests = lengths.shape[0]
    per_group = H // KVH
    slot_count = relaid.shape[2] // requests
    query_heads = query_rows.reshape(requests, kv_count, per_group, HD)
    key_rows = relaid[0].reshape(kv_count, HD, slot_count, requests)
    value_rows = relaid[1].reshape(kv_count, HD, slot_count, requests)
    scores = jnp.einsum(
        "rgtd,gdpr->rgtp", query_heads, key_rows, preferred_element_type=jnp.float32
    ) * (1.0 / math.sqrt(HD))
    alive_mask = (positions[None, :] < lengths[:, None])[:, None, None, :]
    highest = jnp.max(jnp.where(alive_mask, scores, -1e30), axis=-1)
    weights = jnp.where(alive_mask, jnp.exp(scores - highest[..., None]), 0.0)
    summed = jnp.einsum(
        "rgtp,gdpr->rgtd",
        weights.astype(jnp.bfloat16),
        value_rows,
        preferred_element_type=jnp.float32,
    )
    return (highest, jnp.sum(weights, axis=-1), summed)


def on_device(
    residual,
    queries,
    new_entries,
    kv_cache,
    lengths,
    routing,
    w_out,
    norm_gain,
    router,
    w_gate,
    w_up,
    w_down,
):
    requests = lengths.shape[0]
    seq_count = lax.axis_size("seq")
    core_count = lax.axis_size("expert")
    seq_index = lax.axis_index("seq")
    core_index = lax.axis_index("expert")
    half_ctx = kv_cache.shape[2] // requests
    ctx_dev = half_ctx // seq_count
    own_heads = KVH // core_count
    relaid = lax.all_to_all(kv_cache, "seq", split_axis=2, concat_axis=1, tiled=True)
    positions = core_index * half_ctx + seq_index * ctx_dev + jnp.arange(ctx_dev, dtype=jnp.int32)
    all_queries = lax.all_gather(queries, "expert", axis=1, tiled=True)
    partials = partial_attention(all_queries, relaid, positions, lengths, KVH)
    merged = combined_all(partials, ("seq", "expert"), merge_parts)
    head_start = core_index * own_heads
    highest = lax.dynamic_slice_in_dim(merged[0], head_start, own_heads, 1)
    totals = lax.dynamic_slice_in_dim(merged[1], head_start, own_heads, 1)
    summed = lax.dynamic_slice_in_dim(merged[2], head_start, own_heads, 1)
    per_group = H // KVH
    query_heads = queries.reshape(requests, own_heads, per_group, HD)
    new_keys = new_entries[0].reshape(requests, own_heads, HD)
    new_values = new_entries[1].reshape(requests, own_heads, HD).astype(jnp.float32)
    own_score = jnp.einsum(
        "rgtd,rgd->rgt", query_heads, new_keys, preferred_element_type=jnp.float32
    ) * (1.0 / math.sqrt(HD))
    joined = jnp.maximum(highest, own_score)
    fade_old = jnp.exp(highest - joined)
    own_weight = jnp.exp(own_score - joined)
    numerator = summed * fade_old[..., None] + own_weight[..., None] * new_values[:, :, None, :]
    denominator = totals * fade_old + own_weight
    attn_rows = (
        (numerator / denominator[..., None])
        .reshape(requests, own_heads * per_group * HD)
        .astype(jnp.bfloat16)
    )
    head_terms = jnp.dot(attn_rows, w_out, preferred_element_type=jnp.float32)
    attended = (residual.astype(jnp.float32) + lax.psum(head_terms, "expert")).astype(jnp.bfloat16)
    gathered = lax.all_gather(attended, "seq", axis=1, tiled=True)
    widened = gathered.astype(jnp.float32)
    mean_square = jnp.mean(widened * widened, axis=-1, keepdims=True)
    normed = (widened * lax.rsqrt(mean_square + 1e-05) * norm_gain.astype(jnp.float32)).astype(
        jnp.bfloat16
    )
    logits = jnp.dot(normed, router, preferred_element_type=jnp.float32)
    expert_total = router.shape[1]
    picked = (
        routing[:, :, None] == jnp.arange(expert_total, dtype=jnp.int32)[None, None, :]
    ).astype(jnp.float32)
    chosen = jnp.sum(picked * logits[:, None, :], axis=-1)
    first_share = jax.nn.sigmoid(chosen[:, 0] - chosen[:, 1])
    shares = jnp.stack([first_share, 1.0 - first_share], axis=-1)
    combine = jnp.sum(picked * shares[:, :, None], axis=1)
    local_ids = core_index * w_gate.shape[0] + jnp.arange(w_gate.shape[0], dtype=jnp.int32)
    select = (jnp.arange(expert_total, dtype=jnp.int32)[:, None] == local_ids[None, :]).astype(
        jnp.float32
    )
    local_share = jnp.sum(combine[:, :, None] * select[None, :, :], axis=1)
    gate_proj = jnp.einsum("rd,edf->ref", normed, w_gate, preferred_element_type=jnp.float32)
    upward = jnp.einsum("rd,edf->ref", normed, w_up, preferred_element_type=jnp.float32)
    activation = (jax.nn.silu(gate_proj) * upward * local_share[:, :, None]).astype(jnp.bfloat16)
    expert_terms = jnp.einsum("ref,efd->rd", activation, w_down, preferred_element_type=jnp.float32)
    reduced = lax.psum_scatter(expert_terms, "seq", scatter_dimension=1, tiled=True)
    expert_out = lax.psum(reduced, "expert").astype(jnp.bfloat16)
    return (attended, expert_out)


def fused_kernel(
    seq_count,
    lengths_in,
    routing_in,
    residual,
    queries,
    new_entries,
    kv_cache,
    w_out,
    gain,
    router,
    w_gate,
    w_up,
    w_down,
    outs,
    k_buf,
    v_buf,
    wo_buf,
    gu_buf,
    wd_buf,
    router_buf,
    gain_buf,
    res_buf,
    new_buf,
    q_buf,
    q_rows,
    kn_rows,
    vn_rows,
    part_mine,
    part_other,
    attn_rows,
    attn_buf,
    proj_mine,
    proj_other,
    att_buf,
    red_send,
    red_buf,
    lengths,
    routing,
    load_sems,
    q_sems,
    part_sems,
    attn_send,
    attn_recv,
    proj_sems,
    att_send,
    att_recv,
    down_send,
    down_recv,
):
    s = lax.axis_index("seq")
    c = lax.axis_index("expert")
    requests, width = residual.shape
    per_group = H // KVH
    rows = requests * per_group
    columns = kv_cache.shape[2]
    own_heads = KVH // 2
    experts, features, hidden = w_gate.shape
    owner_core = s // own_heads
    slot = lax.rem(s, own_heads)
    is_owner = c == owner_core
    other = {"expert": 1 - c}
    remote = functools.partial(
        pltpu.make_async_remote_copy, device_id_type=pl.DeviceIdType.MESH
    )

    head_span = per_group * HD
    q_cols = pl.ds(pl.multiple_of(slot * head_span, HD), head_span)
    n_cols = pl.ds(pl.multiple_of(slot * HD, HD), HD)
    load_q = pltpu.make_async_copy(queries.at[:, q_cols], q_buf, load_sems.at[0])
    load_new = pltpu.make_async_copy(new_entries.at[:, :, n_cols], new_buf, load_sems.at[1])
    load_k = pltpu.make_async_copy(kv_cache.at[0], k_buf, load_sems.at[2])
    load_v = pltpu.make_async_copy(kv_cache.at[1], v_buf, load_sems.at[3])
    load_wo = [
        pltpu.make_async_copy(
            w_out.at[pl.ds(h * head_span, head_span)], wo_buf.at[h], load_sems.at[4 + h]
        )
        for h in range(own_heads)
    ]
    at = 4 + own_heads
    load_res = pltpu.make_async_copy(residual, res_buf, load_sems.at[at])
    load_gain = pltpu.make_async_copy(gain, gain_buf, load_sems.at[at + 1])
    load_router = pltpu.make_async_copy(router, router_buf, load_sems.at[at + 2])
    load_gu = []
    load_wd = []
    for e in range(experts):
        for i, w in enumerate((w_gate, w_up)):
            load_gu.append(
                pltpu.make_async_copy(
                    w.at[e],
                    gu_buf.at[:, pl.ds((2 * e + i) * hidden, hidden)],
                    load_sems.at[at + 3],
                )
            )
        load_wd.append(
            pltpu.make_async_copy(
                w_down.at[e], wd_buf.at[pl.ds(e * hidden, hidden)], load_sems.at[at + 4]
            )
        )

    @pl.when(is_owner)
    def _():
        load_q.start()
        load_new.start()

    load_lengths = pltpu.make_async_copy(lengths_in, lengths, load_sems.at[at + 5])
    load_routing = pltpu.make_async_copy(routing_in, routing, load_sems.at[at + 6])
    load_lengths.start()
    load_routing.start()
    load_k.start()
    load_v.start()
    for load in load_wo:
        load.start()
    load_res.start()
    load_gain.start()
    load_router.start()
    for load in load_gu + load_wd:
        load.start()

    barrier = pltpu.get_barrier_semaphore()
    pl.semaphore_signal(barrier, inc=1, device_id=other, device_id_type=pl.DeviceIdType.MESH)
    for step in range(1, seq_count):
        peer = lax.rem(s + step, seq_count)
        for core in range(2):
            pl.semaphore_signal(
                barrier,
                inc=1,
                device_id={"seq": peer, "expert": core},
                device_id_type=pl.DeviceIdType.MESH,
            )
    pl.semaphore_wait(barrier, 2 * seq_count - 1)

    send_q = remote(
        src_ref=queries.at[:, q_cols],
        dst_ref=q_buf,
        send_sem=q_sems.at[0],
        recv_sem=q_sems.at[1],
        device_id=other,
    )

    @pl.when(is_owner)
    def _():
        send_q.start()
        load_q.wait()
        load_new.wait()

    @pl.when(jnp.logical_not(is_owner))
    def _():
        send_q.wait_recv()

    for t in range(per_group):
        q_rows[pl.ds(t * requests, requests), :] = q_buf[:, pl.ds(t * HD, HD)].astype(jnp.float32)
    q_f32 = q_rows[...]
    scale = 1.0 / math.sqrt(HD)
    load_k.wait()
    load_lengths.wait()
    load_routing.wait()
    scores = (
        jnp.dot(q_f32.astype(jnp.bfloat16), k_buf[...], preferred_element_type=jnp.float32) * scale
    )
    row_id = lax.broadcasted_iota(jnp.int32, (rows, 1), 0)
    row_req = lax.rem(row_id, requests)
    limit = jnp.zeros((rows, 1), jnp.int32)
    for r in range(requests):
        limit = jnp.where(row_req == r, lengths[r], limit)
    limit = limit * requests - c * columns
    col_id = lax.broadcasted_iota(jnp.int32, (rows, columns), 1)
    alive = ((col_id & (requests - 1)) == row_req) & (col_id < limit)
    scores = jnp.where(alive, scores, -1e30)
    highest = jnp.max(scores, axis=-1, keepdims=True)
    weights = jnp.where(alive, jnp.exp(scores - highest), 0.0)
    total = jnp.sum(weights, axis=-1, keepdims=True)
    load_v.wait()
    summed = lax.dot_general(
        weights.astype(jnp.bfloat16),
        v_buf[...],
        (((1,), (1,)), ((), ())),
        preferred_element_type=jnp.float32,
    )

    send_part = remote(
        src_ref=part_mine,
        dst_ref=part_other,
        send_sem=part_sems.at[0],
        recv_sem=part_sems.at[1],
        device_id=other,
    )
    attn_copies = []
    for step in range(1, seq_count):
        peer = lax.rem(s + step, seq_count)
        attn_copies.append(
            remote(
                src_ref=attn_buf.at[slot],
                dst_ref=attn_buf.at[slot],
                send_sem=attn_send,
                recv_sem=attn_recv.at[slot],
                device_id={"seq": peer},
            )
        )

    lane = lax.broadcasted_iota(jnp.int32, (rows, HD), 1)

    @pl.when(jnp.logical_not(is_owner))
    def _():
        part_mine[0] = summed
        part_mine[1] = jnp.where(lane < HD // 2, highest, total)
        send_part.start()

    @pl.when(is_owner)
    def _():
        for t in range(per_group):
            kn_rows[pl.ds(t * requests, requests), :] = new_buf[0].astype(jnp.float32)
            vn_rows[pl.ds(t * requests, requests), :] = new_buf[1].astype(jnp.float32)
        own = jnp.sum(q_f32 * kn_rows[...], axis=-1, keepdims=True) * scale
        mine = jnp.maximum(highest, own)
        send_part.wait_recv()
        stats = part_other[1]
        high_other = stats[:, 0:1]
        total_other = stats[:, HD - 1 : HD]
        joined = jnp.maximum(mine, high_other)
        fade = jnp.exp(highest - joined)
        fade_other = jnp.exp(high_other - joined)
        own_weight = jnp.exp(own - joined)
        numer = summed * fade + part_other[0] * fade_other + own_weight * vn_rows[...]
        denom = total * fade + total_other * fade_other + own_weight
        attn_rows[...] = numer / denom
        for t in range(per_group):
            attn_buf[slot, :, pl.ds(t * HD, HD)] = attn_rows[
                pl.ds(t * requests, requests), :
            ].astype(jnp.bfloat16)
        for copy in attn_copies:
            copy.start()

    for h in range(own_heads):
        load_wo[h].wait()

        @pl.when(jnp.logical_not(is_owner & (slot == h)))
        def _():
            remote(
                src_ref=attn_buf.at[h],
                dst_ref=attn_buf.at[h],
                send_sem=attn_send,
                recv_sem=attn_recv.at[h],
                device_id=other,
            ).wait_recv()

    proj = jnp.dot(
        jnp.concatenate([attn_buf[h] for h in range(own_heads)], axis=1),
        wo_buf[...].reshape(own_heads * head_span, width),
        preferred_element_type=jnp.float32,
    )
    proj_mine[...] = proj
    send_proj = remote(
        src_ref=proj_mine,
        dst_ref=proj_other,
        send_sem=proj_sems.at[0],
        recv_sem=proj_sems.at[1],
        device_id=other,
    )
    send_proj.start()
    load_res.wait()
    load_gain.wait()
    load_router.wait()
    for load in load_gu:
        load.wait()
    res_f32 = res_buf[...].astype(jnp.float32)
    send_proj.wait_recv()
    attended = (res_f32 + (proj + proj_other[...])).astype(jnp.bfloat16)
    att_buf[s] = attended
    outs[0] = attended
    att_copies = []
    for step in range(1, seq_count):
        peer = lax.rem(s + step, seq_count)
        att_copies.append(
            remote(
                src_ref=att_buf.at[s],
                dst_ref=att_buf.at[s],
                send_sem=att_send,
                recv_sem=att_recv.at[s],
                device_id={"seq": peer},
            )
        )
    for copy in att_copies:
        copy.start()

    for i in range(seq_count):

        @pl.when(s != i)
        def _():
            remote(
                src_ref=att_buf.at[i],
                dst_ref=att_buf.at[i],
                send_sem=att_send,
                recv_sem=att_recv.at[i],
                device_id=other,
            ).wait_recv()

    x = jnp.concatenate([att_buf[i] for i in range(seq_count)], axis=1).astype(jnp.float32)
    scaled = (x * gain_buf[...].astype(jnp.float32)[None, :]).astype(jnp.bfloat16)
    gu = jnp.dot(scaled, gu_buf[...], preferred_element_type=jnp.float32)
    squares = jnp.sum(x * x, axis=-1, keepdims=True)
    logits = lax.dot_general(
        scaled, router_buf[...], (((1,), (1,)), ((), ())), preferred_element_type=jnp.float32
    )
    inverse = lax.rsqrt(squares * (1.0 / features) + 1e-05)
    logits = logits * inverse
    gu = gu * inverse
    req_id = lax.broadcasted_iota(jnp.int32, (requests, 1), 0)
    first_id = jnp.zeros((requests, 1), jnp.int32)
    second_id = jnp.zeros((requests, 1), jnp.int32)
    for r in range(requests):
        first_id = jnp.where(req_id == r, routing[0, r], first_id)
        second_id = jnp.where(req_id == r, routing[1, r], second_id)
    expert_id = lax.broadcasted_iota(jnp.int32, logits.shape, 1)
    gap = jnp.sum(
        jnp.where(expert_id == first_id, logits, 0.0)
        - jnp.where(expert_id == second_id, logits, 0.0),
        axis=-1,
        keepdims=True,
    )
    first_share = 1.0 / (1.0 + jnp.exp(-gap))
    acts = []
    for e in range(experts):
        number = c * experts + e
        share = jnp.where(number == first_id, first_share, 0.0) + jnp.where(
            number == second_id, 1.0 - first_share, 0.0
        )
        gate = gu[:, 2 * e * hidden : (2 * e + 1) * hidden]
        up = gu[:, (2 * e + 1) * hidden : (2 * e + 2) * hidden]
        acts.append((gate / (1.0 + jnp.exp(-gate)) * up * share).astype(jnp.bfloat16))
    act = jnp.concatenate(acts, axis=1)
    for load in load_wd:
        load.wait()

    me = s * 2 + c
    down_copies = []
    steps = sorted(range(seq_count), key=lambda step: -min(step, seq_count - step))
    half = seq_count // 2
    for group in (steps[:half], steps[half:]):
        blocks = []
        for step in group:
            peer = lax.rem(s + step, seq_count)
            block = jnp.dot(
                act,
                wd_buf[:, pl.ds(pl.multiple_of(peer * width, HD), width)],
                preferred_element_type=jnp.float32,
            )
            blocks.append(block.astype(jnp.bfloat16))
        for step, block in zip(group, blocks):
            if step:
                red_send[step - 1] = block
            else:
                red_buf[me] = block
        for step in group:
            peer = lax.rem(s + step, seq_count)
            for core in range(2):
                target = {"seq": peer, "expert": core} if step else other
                if step or core:
                    copy = remote(
                        src_ref=red_send.at[step - 1] if step else red_buf.at[me],
                        dst_ref=red_buf.at[me],
                        send_sem=down_send,
                        recv_sem=down_recv.at[me],
                        device_id=target,
                    )
                    copy.start()
                    down_copies.append(copy)
    for i in range(2 * seq_count):

        @pl.when(me != i)
        def _():
            remote(
                src_ref=red_buf.at[i],
                dst_ref=red_buf.at[i],
                send_sem=down_send,
                recv_sem=down_recv.at[i],
                device_id=other,
            ).wait_recv()

    result = jnp.sum(red_buf[...].astype(jnp.float32), axis=0)
    outs[1] = result.astype(jnp.bfloat16)

    @pl.when(is_owner)
    def _():
        send_q.wait_send()
        for copy in attn_copies:
            copy.wait_send()

    @pl.when(jnp.logical_not(is_owner))
    def _():
        send_part.wait_send()

    send_proj.wait_send()
    for copy in att_copies + down_copies:
        copy.wait_send()


def fused_step(
    residual,
    queries,
    new_entries,
    kv_cache,
    lengths,
    routing,
    w_out,
    norm_gain,
    router,
    w_gate,
    w_up,
    w_down,
):
    seq_count = lax.axis_size("seq")
    requests, width = residual.shape
    per_group = H // KVH
    own_heads = KVH // 2
    rows = requests * per_group
    columns = kv_cache.shape[2]
    experts, features, hidden = w_gate.shape
    bf16, f32 = jnp.bfloat16, jnp.float32
    vmem = pltpu.VMEM
    dma = pltpu.SemaphoreType.DMA
    anywhere = pl.BlockSpec(memory_space=pltpu.HBM)
    outs = pl.pallas_call(
        functools.partial(fused_kernel, seq_count),
        out_shape=pltpu.VMEM((2, requests, width), bf16),
        in_specs=[anywhere] * 12,
        out_specs=pl.BlockSpec(memory_space=vmem),
        scratch_shapes=[
            vmem((HD, columns), bf16),
            vmem((HD, columns), bf16),
            vmem((own_heads, per_group * HD, width), bf16),
            vmem((features, 2 * experts * hidden), bf16),
            vmem((experts * hidden, features), bf16),
            vmem((router.shape[1], features), bf16),
            vmem((features,), bf16),
            vmem((requests, width), bf16),
            vmem((2, requests, HD), bf16),
            vmem((requests, per_group * HD), bf16),
            vmem((rows, HD), f32),
            vmem((rows, HD), f32),
            vmem((rows, HD), f32),
            vmem((2, rows, HD), f32),
            vmem((2, rows, HD), f32),
            vmem((rows, HD), f32),
            vmem((own_heads, requests, per_group * HD), bf16),
            vmem((requests, width), f32),
            vmem((requests, width), f32),
            vmem((seq_count, requests, width), bf16),
            vmem((seq_count, requests, width), bf16),
            vmem((2 * seq_count, requests, width), bf16),
            pltpu.SMEM((requests,), jnp.int32),
            pltpu.SMEM((2, requests), jnp.int32),
            dma((11 + own_heads,)),
            dma((2,)),
            dma((2,)),
            dma,
            dma((own_heads,)),
            dma((2,)),
            dma,
            dma((seq_count,)),
            dma,
            dma((2 * seq_count,)),
        ],
        compiler_params=pltpu.CompilerParams(
            collective_id=0, has_side_effects=True, vmem_limit_bytes=60 * 1024 * 1024
        ),
        name="decode_step",
    )(
        lengths,
        routing.T,
        residual,
        queries,
        new_entries,
        kv_cache,
        w_out,
        norm_gain,
        router.T,
        w_gate,
        w_up,
        w_down,
    )
    return (outs[0], outs[1])


def step_on_device(*args):
    kv_cache, lengths = args[3], args[4]
    requests = lengths.shape[0]
    whole_head = kv_cache.shape[1] == HD and lax.axis_size("seq") == KVH
    if whole_head and lax.axis_size("expert") == 2 and requests & (requests - 1) == 0:
        return fused_step(*args)
    return on_device(*args)


def solution(mesh):
    in_specs = (
        P("groups", "seq"),
        P("groups", "expert"),
        P(None, "groups", "expert"),
        P(None, "seq", ("groups", "expert")),
        P("groups"),
        P("groups", None),
        P("expert", "seq"),
        P(),
        P(),
        P("expert", None, "seq"),
        P("expert", None, "seq"),
        P("expert", "seq", None),
    )
    out_specs = (P("groups", "seq"), P("groups", "seq"))
    return jax.shard_map(
        step_on_device, mesh=mesh, in_specs=in_specs, out_specs=out_specs, check_vma=False
    )
```

```python
import functools
import math

import jax
import jax.numpy as jnp
from jax import lax
from jax.experimental import pallas as pl
from jax.experimental.pallas import tpu as pltpu
from jax.sharding import PartitionSpec as P

H = 48
KVH = 8
HD = 128


def combined_all(value, axis, join):
    pieces = jax.tree.map(lambda part: lax.all_gather(part, axis), value)
    head = jax.tree.map(lambda part: part[0], pieces)
    tail = jax.tree.map(lambda part: part[1:], pieces)
    running, _ = lax.scan(lambda running, share: (join(running, share), None), head, tail)
    return running


def merge_parts(earlier, later):
    high_left, total_left, sum_left = earlier
    high_right, total_right, sum_right = later
    joined = jnp.maximum(high_left, high_right)
    scale_left = jnp.exp(high_left - joined)
    scale_right = jnp.exp(high_right - joined)
    return (
        joined,
        total_left * scale_left + total_right * scale_right,
        sum_left * scale_left[..., None] + sum_right * scale_right[..., None],
    )


def partial_attention(query_rows, relaid, positions, lengths, kv_count):
    requests = lengths.shape[0]
    per_group = H // KVH
    slot_count = relaid.shape[2] // requests
    query_heads = query_rows.reshape(requests, kv_count, per_group, HD)
    key_rows = relaid[0].reshape(kv_count, HD, slot_count, requests)
    value_rows = relaid[1].reshape(kv_count, HD, slot_count, requests)
    scores = jnp.einsum(
        "rgtd,gdpr->rgtp", query_heads, key_rows, preferred_element_type=jnp.float32
    ) * (1.0 / math.sqrt(HD))
    alive_mask = (positions[None, :] < lengths[:, None])[:, None, None, :]
    highest = jnp.max(jnp.where(alive_mask, scores, -1e30), axis=-1)
    weights = jnp.where(alive_mask, jnp.exp(scores - highest[..., None]), 0.0)
    summed = jnp.einsum(
        "rgtp,gdpr->rgtd",
        weights.astype(jnp.bfloat16),
        value_rows,
        preferred_element_type=jnp.float32,
    )
    return (highest, jnp.sum(weights, axis=-1), summed)


def on_device(
    residual,
    queries,
    new_entries,
    kv_cache,
    lengths,
    routing,
    w_out,
    norm_gain,
    router,
    w_gate,
    w_up,
    w_down,
):
    requests = lengths.shape[0]
    seq_count = lax.axis_size("seq")
    core_count = lax.axis_size("expert")
    seq_index = lax.axis_index("seq")
    core_index = lax.axis_index("expert")
    half_ctx = kv_cache.shape[2] // requests
    ctx_dev = half_ctx // seq_count
    own_heads = KVH // core_count
    relaid = lax.all_to_all(kv_cache, "seq", split_axis=2, concat_axis=1, tiled=True)
    positions = core_index * half_ctx + seq_index * ctx_dev + jnp.arange(ctx_dev, dtype=jnp.int32)
    all_queries = lax.all_gather(queries, "expert", axis=1, tiled=True)
    partials = partial_attention(all_queries, relaid, positions, lengths, KVH)
    merged = combined_all(partials, ("seq", "expert"), merge_parts)
    head_start = core_index * own_heads
    highest = lax.dynamic_slice_in_dim(merged[0], head_start, own_heads, 1)
    totals = lax.dynamic_slice_in_dim(merged[1], head_start, own_heads, 1)
    summed = lax.dynamic_slice_in_dim(merged[2], head_start, own_heads, 1)
    per_group = H // KVH
    query_heads = queries.reshape(requests, own_heads, per_group, HD)
    new_keys = new_entries[0].reshape(requests, own_heads, HD)
    new_values = new_entries[1].reshape(requests, own_heads, HD).astype(jnp.float32)
    own_score = jnp.einsum(
        "rgtd,rgd->rgt", query_heads, new_keys, preferred_element_type=jnp.float32
    ) * (1.0 / math.sqrt(HD))
    joined = jnp.maximum(highest, own_score)
    fade_old = jnp.exp(highest - joined)
    own_weight = jnp.exp(own_score - joined)
    numerator = summed * fade_old[..., None] + own_weight[..., None] * new_values[:, :, None, :]
    denominator = totals * fade_old + own_weight
    attn_rows = (
        (numerator / denominator[..., None])
        .reshape(requests, own_heads * per_group * HD)
        .astype(jnp.bfloat16)
    )
    head_terms = jnp.dot(attn_rows, w_out, preferred_element_type=jnp.float32)
    attended = (residual.astype(jnp.float32) + lax.psum(head_terms, "expert")).astype(jnp.bfloat16)
    gathered = lax.all_gather(attended, "seq", axis=1, tiled=True)
    widened = gathered.astype(jnp.float32)
    mean_square = jnp.mean(widened * widened, axis=-1, keepdims=True)
    normed = (widened * lax.rsqrt(mean_square + 1e-05) * norm_gain.astype(jnp.float32)).astype(
        jnp.bfloat16
    )
    logits = jnp.dot(normed, router, preferred_element_type=jnp.float32)
    expert_total = router.shape[1]
    picked = (
        routing[:, :, None] == jnp.arange(expert_total, dtype=jnp.int32)[None, None, :]
    ).astype(jnp.float32)
    chosen = jnp.sum(picked * logits[:, None, :], axis=-1)
    first_share = jax.nn.sigmoid(chosen[:, 0] - chosen[:, 1])
    shares = jnp.stack([first_share, 1.0 - first_share], axis=-1)
    combine = jnp.sum(picked * shares[:, :, None], axis=1)
    local_ids = core_index * w_gate.shape[0] + jnp.arange(w_gate.shape[0], dtype=jnp.int32)
    select = (jnp.arange(expert_total, dtype=jnp.int32)[:, None] == local_ids[None, :]).astype(
        jnp.float32
    )
    local_share = jnp.sum(combine[:, :, None] * select[None, :, :], axis=1)
    gate_proj = jnp.einsum("rd,edf->ref", normed, w_gate, preferred_element_type=jnp.float32)
    upward = jnp.einsum("rd,edf->ref", normed, w_up, preferred_element_type=jnp.float32)
    activation = (jax.nn.silu(gate_proj) * upward * local_share[:, :, None]).astype(jnp.bfloat16)
    expert_terms = jnp.einsum("ref,efd->rd", activation, w_down, preferred_element_type=jnp.float32)
    reduced = lax.psum_scatter(expert_terms, "seq", scatter_dimension=1, tiled=True)
    expert_out = lax.psum(reduced, "expert").astype(jnp.bfloat16)
    return (attended, expert_out)


def fused_kernel(
    seq_count,
    lengths_in,
    routing_in,
    residual,
    queries,
    new_entries,
    kv_cache,
    w_out,
    gain,
    router,
    w_gate,
    w_up,
    w_down,
    outs,
    k_buf,
    v_buf,
    wo_buf,
    gu_buf,
    wd_buf,
    router_buf,
    gain_buf,
    res_buf,
    new_buf,
    q_buf,
    q_rows,
    kn_rows,
    vn_rows,
    part_mine,
    part_other,
    attn_rows,
    attn_buf,
    proj_mine,
    proj_other,
    att_buf,
    red_send,
    red_buf,
    relay_sems,
    lengths,
    routing,
    load_sems,
    q_sems,
    part_sems,
    attn_send,
    attn_recv,
    proj_sems,
    att_send,
    att_recv,
    down_send,
    down_recv,
):
    s = lax.axis_index("seq")
    c = lax.axis_index("expert")
    requests, width = residual.shape
    per_group = H // KVH
    rows = requests * per_group
    columns = kv_cache.shape[2]
    own_heads = KVH // 2
    experts, features, hidden = w_gate.shape
    owner_core = s // own_heads
    slot = lax.rem(s, own_heads)
    is_owner = c == owner_core
    other = {"expert": 1 - c}
    remote = functools.partial(
        pltpu.make_async_remote_copy, device_id_type=pl.DeviceIdType.MESH
    )

    head_span = per_group * HD
    q_cols = pl.ds(pl.multiple_of(slot * head_span, HD), head_span)
    n_cols = pl.ds(pl.multiple_of(slot * HD, HD), HD)
    load_q = pltpu.make_async_copy(queries.at[:, q_cols], q_buf, load_sems.at[0])
    load_new = pltpu.make_async_copy(new_entries.at[:, :, n_cols], new_buf, load_sems.at[1])
    load_k = pltpu.make_async_copy(kv_cache.at[0], k_buf, load_sems.at[2])
    load_v = pltpu.make_async_copy(kv_cache.at[1], v_buf, load_sems.at[3])
    load_wo = [
        pltpu.make_async_copy(
            w_out.at[pl.ds(h * head_span, head_span)], wo_buf.at[h], load_sems.at[4 + h]
        )
        for h in range(own_heads)
    ]
    at = 4 + own_heads
    load_res = pltpu.make_async_copy(residual, res_buf, load_sems.at[at])
    load_gain = pltpu.make_async_copy(gain, gain_buf, load_sems.at[at + 1])
    load_router = pltpu.make_async_copy(router, router_buf, load_sems.at[at + 2])
    load_gu = []
    load_wd = []
    for e in range(experts):
        for i, w in enumerate((w_gate, w_up)):
            load_gu.append(
                pltpu.make_async_copy(
                    w.at[e],
                    gu_buf.at[:, pl.ds((2 * e + i) * hidden, hidden)],
                    load_sems.at[at + 3],
                )
            )
        load_wd.append(
            pltpu.make_async_copy(
                w_down.at[e], wd_buf.at[pl.ds(e * hidden, hidden)], load_sems.at[at + 4]
            )
        )

    @pl.when(is_owner)
    def _():
        load_q.start()
        load_new.start()

    load_lengths = pltpu.make_async_copy(lengths_in, lengths, load_sems.at[at + 5])
    load_routing = pltpu.make_async_copy(routing_in, routing, load_sems.at[at + 6])
    load_lengths.start()
    load_routing.start()
    load_k.start()
    load_v.start()
    for load in load_wo:
        load.start()
    load_res.start()
    load_gain.start()
    load_router.start()
    for load in load_gu + load_wd:
        load.start()

    has_up = s + 2 < seq_count
    has_down = s >= 2
    signal = functools.partial(pl.semaphore_signal, inc=1, device_id_type=pl.DeviceIdType.MESH)

    def tell_neighbours(sem):
        signal(sem, device_id={"seq": s ^ 1})

        @pl.when(has_up)
        def _():
            signal(sem, device_id={"seq": s + 2})

        @pl.when(has_down)
        def _():
            signal(sem, device_id={"seq": s - 2})

    neighbours = 1 + has_up.astype(jnp.int32) + has_down.astype(jnp.int32)
    barrier = pltpu.get_barrier_semaphore()
    signal(barrier, device_id=other)
    tell_neighbours(barrier)
    pl.semaphore_wait(barrier, neighbours + 1)
    relays = seq_count // 2 - 1
    tell_neighbours(relay_sems.at[0])

    def relay(i):
        pl.semaphore_wait(relay_sems.at[i], neighbours)
        if i + 1 < relays:
            tell_neighbours(relay_sems.at[i + 1])

    send_q = remote(
        src_ref=queries.at[:, q_cols],
        dst_ref=q_buf,
        send_sem=q_sems.at[0],
        recv_sem=q_sems.at[1],
        device_id=other,
    )

    @pl.when(is_owner)
    def _():
        send_q.start()
        load_q.wait()
        load_new.wait()

    @pl.when(jnp.logical_not(is_owner))
    def _():
        send_q.wait_recv()

    for t in range(per_group):
        q_rows[pl.ds(t * requests, requests), :] = q_buf[:, pl.ds(t * HD, HD)].astype(jnp.float32)
    q_f32 = q_rows[...]
    relay(0)
    scale = 1.0 / math.sqrt(HD)
    load_k.wait()
    load_lengths.wait()
    load_routing.wait()
    scores = (
        jnp.dot(q_f32.astype(jnp.bfloat16), k_buf[...], preferred_element_type=jnp.float32) * scale
    )
    row_id = lax.broadcasted_iota(jnp.int32, (rows, 1), 0)
    row_req = lax.rem(row_id, requests)
    limit = jnp.zeros((rows, 1), jnp.int32)
    for r in range(requests):
        limit = jnp.where(row_req == r, lengths[r], limit)
    limit = limit * requests - c * columns
    col_id = lax.broadcasted_iota(jnp.int32, (rows, columns), 1)
    alive = ((col_id & (requests - 1)) == row_req) & (col_id < limit)
    scores = jnp.where(alive, scores, -1e30)
    highest = jnp.max(scores, axis=-1, keepdims=True)
    weights = jnp.where(alive, jnp.exp(scores - highest), 0.0)
    total = jnp.sum(weights, axis=-1, keepdims=True)
    load_v.wait()
    relay(1)
    summed = lax.dot_general(
        weights.astype(jnp.bfloat16),
        v_buf[...],
        (((1,), (1,)), ((), ())),
        preferred_element_type=jnp.float32,
    )

    send_part = remote(
        src_ref=part_mine,
        dst_ref=part_other,
        send_sem=part_sems.at[0],
        recv_sem=part_sems.at[1],
        device_id=other,
    )
    attn_copies = []
    for step in range(1, seq_count):
        peer = lax.rem(s + step, seq_count)
        attn_copies.append(
            remote(
                src_ref=attn_buf.at[slot],
                dst_ref=attn_buf.at[slot],
                send_sem=attn_send,
                recv_sem=attn_recv.at[slot],
                device_id={"seq": peer},
            )
        )

    lane = lax.broadcasted_iota(jnp.int32, (rows, HD), 1)

    @pl.when(jnp.logical_not(is_owner))
    def _():
        part_mine[0] = summed
        part_mine[1] = jnp.where(lane < HD // 2, highest, total)
        send_part.start()
        for i in range(2, relays):
            relay(i)

    @pl.when(is_owner)
    def _():
        for t in range(per_group):
            kn_rows[pl.ds(t * requests, requests), :] = new_buf[0].astype(jnp.float32)
            vn_rows[pl.ds(t * requests, requests), :] = new_buf[1].astype(jnp.float32)
        own = jnp.sum(q_f32 * kn_rows[...], axis=-1, keepdims=True) * scale
        mine = jnp.maximum(highest, own)
        send_part.wait_recv()
        stats = part_other[1]
        high_other = stats[:, 0:1]
        total_other = stats[:, HD - 1 : HD]
        joined = jnp.maximum(mine, high_other)
        fade = jnp.exp(highest - joined)
        fade_other = jnp.exp(high_other - joined)
        own_weight = jnp.exp(own - joined)
        numer = summed * fade + part_other[0] * fade_other + own_weight * vn_rows[...]
        denom = total * fade + total_other * fade_other + own_weight
        attn_rows[...] = numer / denom
        for t in range(per_group):
            attn_buf[slot, :, pl.ds(t * HD, HD)] = attn_rows[
                pl.ds(t * requests, requests), :
            ].astype(jnp.bfloat16)
        for i in range(2, relays):
            relay(i)
        for copy in attn_copies:
            copy.start()

    for h in range(own_heads):
        load_wo[h].wait()

        @pl.when(jnp.logical_not(is_owner & (slot == h)))
        def _():
            remote(
                src_ref=attn_buf.at[h],
                dst_ref=attn_buf.at[h],
                send_sem=attn_send,
                recv_sem=attn_recv.at[h],
                device_id=other,
            ).wait_recv()

    proj = jnp.dot(
        jnp.concatenate([attn_buf[h] for h in range(own_heads)], axis=1),
        wo_buf[...].reshape(own_heads * head_span, width),
        preferred_element_type=jnp.float32,
    )
    proj_mine[...] = proj
    send_proj = remote(
        src_ref=proj_mine,
        dst_ref=proj_other,
        send_sem=proj_sems.at[0],
        recv_sem=proj_sems.at[1],
        device_id=other,
    )
    send_proj.start()
    load_res.wait()
    load_gain.wait()
    load_router.wait()
    for load in load_gu:
        load.wait()
    res_f32 = res_buf[...].astype(jnp.float32)
    send_proj.wait_recv()
    attended = (res_f32 + (proj + proj_other[...])).astype(jnp.bfloat16)
    att_buf[s] = attended
    outs[0] = attended
    att_copies = []
    for step in range(1, seq_count):
        peer = lax.rem(s + step, seq_count)
        att_copies.append(
            remote(
                src_ref=att_buf.at[s],
                dst_ref=att_buf.at[s],
                send_sem=att_send,
                recv_sem=att_recv.at[s],
                device_id={"seq": peer},
            )
        )
    for copy in att_copies:
        copy.start()

    for i in range(seq_count):

        @pl.when(s != i)
        def _():
            remote(
                src_ref=att_buf.at[i],
                dst_ref=att_buf.at[i],
                send_sem=att_send,
                recv_sem=att_recv.at[i],
                device_id=other,
            ).wait_recv()

    x = jnp.concatenate([att_buf[i] for i in range(seq_count)], axis=1).astype(jnp.float32)
    scaled = (x * gain_buf[...].astype(jnp.float32)[None, :]).astype(jnp.bfloat16)
    gu = jnp.dot(scaled, gu_buf[...], preferred_element_type=jnp.float32)
    squares = jnp.sum(x * x, axis=-1, keepdims=True)
    logits = lax.dot_general(
        scaled, router_buf[...], (((1,), (1,)), ((), ())), preferred_element_type=jnp.float32
    )
    inverse = lax.rsqrt(squares * (1.0 / features) + 1e-05)
    logits = logits * inverse
    gu = gu * inverse
    req_id = lax.broadcasted_iota(jnp.int32, (requests, 1), 0)
    first_id = jnp.zeros((requests, 1), jnp.int32)
    second_id = jnp.zeros((requests, 1), jnp.int32)
    for r in range(requests):
        first_id = jnp.where(req_id == r, routing[0, r], first_id)
        second_id = jnp.where(req_id == r, routing[1, r], second_id)
    expert_id = lax.broadcasted_iota(jnp.int32, logits.shape, 1)
    gap = jnp.sum(
        jnp.where(expert_id == first_id, logits, 0.0)
        - jnp.where(expert_id == second_id, logits, 0.0),
        axis=-1,
        keepdims=True,
    )
    first_share = 1.0 / (1.0 + jnp.exp(-gap))
    acts = []
    for e in range(experts):
        number = c * experts + e
        share = jnp.where(number == first_id, first_share, 0.0) + jnp.where(
            number == second_id, 1.0 - first_share, 0.0
        )
        gate = gu[:, 2 * e * hidden : (2 * e + 1) * hidden]
        up = gu[:, (2 * e + 1) * hidden : (2 * e + 2) * hidden]
        acts.append((gate / (1.0 + jnp.exp(-gate)) * up * share).astype(jnp.bfloat16))
    act = jnp.concatenate(acts, axis=1)
    for load in load_wd:
        load.wait()

    me = s * 2 + c
    down_copies = []
    steps = sorted(range(seq_count), key=lambda step: -min(step, seq_count - step))
    half = seq_count // 2
    for group in (steps[:half], steps[half:]):
        blocks = []
        for step in group:
            peer = lax.rem(s + step, seq_count)
            block = jnp.dot(
                act,
                wd_buf[:, pl.ds(pl.multiple_of(peer * width, HD), width)],
                preferred_element_type=jnp.float32,
            )
            blocks.append(block.astype(jnp.bfloat16))
        for step, block in zip(group, blocks):
            if step:
                red_send[step - 1] = block
            else:
                red_buf[me] = block
        for step in group:
            peer = lax.rem(s + step, seq_count)
            for core in range(2):
                target = {"seq": peer, "expert": core} if step else other
                if step or core:
                    copy = remote(
                        src_ref=red_send.at[step - 1] if step else red_buf.at[me],
                        dst_ref=red_buf.at[me],
                        send_sem=down_send,
                        recv_sem=down_recv.at[me],
                        device_id=target,
                    )
                    copy.start()
                    down_copies.append(copy)
    for i in range(2 * seq_count):

        @pl.when(me != i)
        def _():
            remote(
                src_ref=red_buf.at[i],
                dst_ref=red_buf.at[i],
                send_sem=down_send,
                recv_sem=down_recv.at[i],
                device_id=other,
            ).wait_recv()

    result = jnp.sum(red_buf[...].astype(jnp.float32), axis=0)
    outs[1] = result.astype(jnp.bfloat16)

    @pl.when(is_owner)
    def _():
        send_q.wait_send()
        for copy in attn_copies:
            copy.wait_send()

    @pl.when(jnp.logical_not(is_owner))
    def _():
        send_part.wait_send()

    send_proj.wait_send()
    for copy in att_copies + down_copies:
        copy.wait_send()


def fused_step(
    residual,
    queries,
    new_entries,
    kv_cache,
    lengths,
    routing,
    w_out,
    norm_gain,
    router,
    w_gate,
    w_up,
    w_down,
):
    seq_count = lax.axis_size("seq")
    requests, width = residual.shape
    per_group = H // KVH
    own_heads = KVH // 2
    rows = requests * per_group
    columns = kv_cache.shape[2]
    experts, features, hidden = w_gate.shape
    bf16, f32 = jnp.bfloat16, jnp.float32
    vmem = pltpu.VMEM
    dma = pltpu.SemaphoreType.DMA
    anywhere = pl.BlockSpec(memory_space=pltpu.HBM)
    outs = pl.pallas_call(
        functools.partial(fused_kernel, seq_count),
        out_shape=pltpu.VMEM((2, requests, width), bf16),
        in_specs=[anywhere] * 12,
        out_specs=pl.BlockSpec(memory_space=vmem),
        scratch_shapes=[
            vmem((HD, columns), bf16),
            vmem((HD, columns), bf16),
            vmem((own_heads, per_group * HD, width), bf16),
            vmem((features, 2 * experts * hidden), bf16),
            vmem((experts * hidden, features), bf16),
            vmem((router.shape[1], features), bf16),
            vmem((features,), bf16),
            vmem((requests, width), bf16),
            vmem((2, requests, HD), bf16),
            vmem((requests, per_group * HD), bf16),
            vmem((rows, HD), f32),
            vmem((rows, HD), f32),
            vmem((rows, HD), f32),
            vmem((2, rows, HD), f32),
            vmem((2, rows, HD), f32),
            vmem((rows, HD), f32),
            vmem((own_heads, requests, per_group * HD), bf16),
            vmem((requests, width), f32),
            vmem((requests, width), f32),
            vmem((seq_count, requests, width), bf16),
            vmem((seq_count, requests, width), bf16),
            vmem((2 * seq_count, requests, width), bf16),
            pltpu.SemaphoreType.REGULAR((seq_count // 2 - 1,)),
            pltpu.SMEM((requests,), jnp.int32),
            pltpu.SMEM((2, requests), jnp.int32),
            dma((11 + own_heads,)),
            dma((2,)),
            dma((2,)),
            dma,
            dma((own_heads,)),
            dma((2,)),
            dma,
            dma((seq_count,)),
            dma,
            dma((2 * seq_count,)),
        ],
        compiler_params=pltpu.CompilerParams(
            collective_id=0, has_side_effects=True, vmem_limit_bytes=60 * 1024 * 1024
        ),
        name="decode_step",
    )(
        lengths,
        routing.T,
        residual,
        queries,
        new_entries,
        kv_cache,
        w_out,
        norm_gain,
        router.T,
        w_gate,
        w_up,
        w_down,
    )
    return (outs[0], outs[1])


def step_on_device(*args):
    kv_cache, lengths = args[3], args[4]
    requests = lengths.shape[0]
    whole_head = kv_cache.shape[1] == HD and lax.axis_size("seq") == KVH
    if whole_head and lax.axis_size("expert") == 2 and requests & (requests - 1) == 0:
        return fused_step(*args)
    return on_device(*args)


def solution(mesh):
    in_specs = (
        P("groups", "seq"),
        P("groups", "expert"),
        P(None, "groups", "expert"),
        P(None, "seq", ("groups", "expert")),
        P("groups"),
        P("groups", None),
        P("expert", "seq"),
        P(),
        P(),
        P("expert", None, "seq"),
        P("expert", None, "seq"),
        P("expert", "seq", None),
    )
    out_specs = (P("groups", "seq"), P("groups", "seq"))
    return jax.shard_map(
        step_on_device, mesh=mesh, in_specs=in_specs, out_specs=out_specs, check_vma=False
    )
```
